32 devices in a mesh: dp: 8 (over z, core), section: 4 (over y, x).
Axes of the slice: x: 2, y: 2, z: 4, core: 2. Of those that a mesh axis runs over, the one named last changes fastest.
Arguments:
- layer_inputs: bfloat16 [4, 2, 16, 32, 4096], P('section', None, 'dp'), may hold values from -6 to 6
- saved_queries: bfloat16 [4, 2, 16, 32, 128], P('section', None, 'dp'), may hold values from -16 to 16
- saved_keys: bfloat16 [4, 2, 16, 32, 128], P('section', None, 'dp'), may hold values from -16 to 16
- held_weights: bfloat16 [4, 2, 2, 4096, 128], P('section'), may hold values from -0.15625 to 0.15625
- cotangent: bfloat16 [2, 16, 32, 4096], P(None, 'dp'), may hold values from -6 to 6
- valid_lengths: int32 [2, 16], P(None, 'dp'), may hold values from 2 to 32, as said below
Outputs:
- input_grads: bfloat16 [4, 2, 16, 32, 4096], P('section', None, 'dp')
- weight_grads: float32 [4, 2, 4096, 128], P('section', None, 'dp')
The draws below stay inside these ranges and needn't reach their ends.
Inputs may be any that keep to these rules, and one draw needn't show every extreme that they name: `valid_lengths`: some sequence has 32 valid tokens.
All inputs are finite; a program needn't handle non-finite values.
Results may differ from the reference program's by a relative error of at most 0.014.
Values may be sent and summed in bfloat16 or wider, within the bound.
No kernel may reach another device: no remote copies, remote signals or barrier semaphores. Data moves between devices by JAX's collectives and lax.ppermute only.
A program may use at most 64 MiB of HBM per device.

```python
import math
import jax
import jax.numpy as jnp
from jax import lax

D = 4096
HEAD = 128
LEN = 32
BATCH = 16
N_SECTION = 4


def draw_pair(key):
    shape = (N_SECTION, 2, BATCH, LEN, HEAD)
    query_key, key_key = jax.random.split(jax.random.fold_in(key, 11), 2)
    queries = jax.random.normal(query_key, shape, jnp.float32)
    key_vectors = jax.random.normal(key_key, shape, jnp.float32)
    return (queries, key_vectors)


def draw_saved_queries(key, part):
    return draw_pair(key)[0].astype(jnp.bfloat16)


def draw_saved_keys(key, part):
    return draw_pair(key)[1].astype(jnp.bfloat16)


def draw_valid_lengths(key, part):
    drawn = jax.random.randint(jax.random.fold_in(key, 3), (2, BATCH), 2, LEN + 1)
    return drawn.at[0, 0].set(LEN).astype(jnp.int32)


def steps_of(rng, extent, cuts, least, high):
    def one(axis_at, blocks):
        heights = jax.random.uniform(jax.random.fold_in(jax.random.fold_in(rng, 6), axis_at), (blocks,), jnp.float32, least / len(cuts), high / len(cuts))
        return jnp.repeat(jnp.exp(heights), extent[axis_at] // blocks).reshape((-1,) + (1,) * (len(extent) - axis_at - 1))

    factor_of = one(*cuts[0])
    for cut in cuts[1:]:
        factor_of = factor_of * one(*cut)
    return factor_of


def centred(rng, extent, scale, bound, cuts=(), kind=jnp.bfloat16):
    factor_of = steps_of(rng, extent, cuts, -0.22, 0.18) if cuts else 1.0
    values = jax.random.normal(rng, extent, jnp.float32) * scale * factor_of
    return jnp.minimum(jnp.maximum(values, -bound), bound).astype(kind)


def setup_inputs(seed: int = 0) -> dict:
    streams_of = jax.random.split(jax.random.key(seed), 7)
    return {
        "layer_inputs": centred(streams_of[0], (N_SECTION, 2, BATCH, LEN, D), 1.0, 6.0, ((0, 4), (2, 8))),
        "saved_queries": draw_saved_queries(jax.random.fold_in(streams_of[6], 71), 0),
        "saved_keys": draw_saved_keys(jax.random.fold_in(streams_of[6], 71), 0),
        "held_weights": centred(streams_of[3], (N_SECTION, 2, 2, D, HEAD), (2 * (D * HEAD) ** 0.5) ** -0.5, 0.15625, ((0, 4),)),
        "cotangent": centred(streams_of[4], (2, BATCH, LEN, D), 1.0, 6.0, ((1, 8),)),
        "valid_lengths": draw_valid_lengths(jax.random.fold_in(streams_of[6], 71), 0),
    }


def attention_weights(queries, key_vectors, valid_lengths):
    length = queries.shape[-2]
    scores = jnp.einsum('...th,...sh->...ts', queries.astype(jnp.float32), key_vectors.astype(jnp.float32)) / math.sqrt(queries.shape[-1])
    row_pos = lax.broadcasted_iota(jnp.int32, (length, length), 0)
    col_pos = lax.broadcasted_iota(jnp.int32, (length, length), 1)
    allowed = (col_pos <= row_pos) & (col_pos < valid_lengths[..., None, None])
    scores = jnp.where(allowed, scores, -jnp.inf)
    row_max = lax.optimization_barrier(jnp.max(scores, axis=-1, keepdims=True))
    raised = jnp.where(allowed, jnp.exp(scores - row_max), 0.0)
    return (raised / lax.optimization_barrier(jnp.sum(raised, axis=-1, keepdims=True))).astype(jnp.bfloat16)

def head_backward(inputs, queries, key_vectors, lengths_now, value_w, output_w, upstream):
    attend = attention_weights(queries, key_vectors, lengths_now)
    seq_count, length, model_width = inputs.shape
    head_size = value_w.shape[1]
    flat_in = inputs.reshape(seq_count * length, model_width)
    flat_up = upstream.reshape(seq_count * length, model_width)
    values = jnp.dot(flat_in, value_w, preferred_element_type=jnp.float32).astype(jnp.bfloat16)
    values = values.reshape(seq_count, length, head_size)
    mixture = jnp.einsum('bts,bsh->bth', attend.astype(jnp.float32), values.astype(jnp.float32)).astype(jnp.bfloat16)
    out_grad = jnp.dot(flat_up, output_w, preferred_element_type=jnp.float32).astype(jnp.bfloat16)
    out_grad = out_grad.reshape(seq_count, length, head_size)
    val_grad = jnp.einsum('bts,bth->bsh', attend.astype(jnp.float32), out_grad.astype(jnp.float32)).astype(jnp.bfloat16)
    flat_vg = val_grad.reshape(seq_count * length, head_size)
    branch = jnp.dot(flat_vg, value_w.T, preferred_element_type=jnp.float32).reshape(seq_count, length, model_width)
    grad_input = (upstream.astype(jnp.float32) + branch).astype(jnp.bfloat16)
    grad_value = jnp.dot(flat_in.T, flat_vg, preferred_element_type=jnp.float32)
    grad_output = jnp.dot(flat_up.T, mixture.reshape(seq_count * length, head_size), preferred_element_type=jnp.float32)
    return (grad_input, grad_value, grad_output)

def reference(layer_inputs, saved_queries, saved_keys, held_weights, cotangent, valid_lengths):
    sections = layer_inputs.shape[0]
    grads_in = [[None] * sections, [None] * sections]
    value_terms = [[None] * sections, [None] * sections]
    output_terms = [[None] * sections, [None] * sections]
    for direction in range(2):
        upstream = cotangent[direction]
        visiting = range(sections - 1, -1, -1) if direction == 0 else range(sections)
        for section_no in visiting:
            grad_input, grad_value, grad_output = head_backward(layer_inputs[section_no, direction], saved_queries[section_no, direction], saved_keys[section_no, direction], valid_lengths[direction], held_weights[section_no, direction, 0], held_weights[section_no, direction, 1], upstream)
            grads_in[direction][section_no] = grad_input
            value_terms[direction][section_no] = grad_value
            output_terms[direction][section_no] = grad_output
            upstream = grad_input
    input_grads = jnp.stack([jnp.stack([grads_in[0][section_no], grads_in[1][section_no]]) for section_no in range(sections)])
    weight_grads = jnp.stack([jnp.stack([value_terms[0][section_no] + value_terms[1][sections - 1 - section_no], output_terms[0][section_no] + output_terms[1][sections - 1 - section_no]]) for section_no in range(sections)])
    return (input_grads, weight_grads)
```

```python
import functools
import math

import jax
import jax.numpy as jnp
from jax import lax
from jax.experimental import pallas as pl
from jax.experimental.pallas import tpu as pltpu
from jax.sharding import PartitionSpec as P


def passed_along(block, axis, distance):
    devices = range(lax.axis_size(axis))
    route = [(i - distance, i) for i in devices if i - distance in devices]
    return lax.ppermute(block, axis, route)


def from_partner(block, axis, bit):
    count = lax.axis_size(axis)
    route = []
    for low in range(count):
        high = low | 1 << bit
        if high != low and high < count:
            route += [(low, high), (high, low)]
    return lax.ppermute(block, axis, route)


def attention_weights(queries, key_vectors, valid_lengths):
    length = queries.shape[-2]
    scores = jnp.einsum(
        "nmth,nmsh->nmts", queries, key_vectors, preferred_element_type=jnp.float32
    ) / math.sqrt(queries.shape[-1])
    row_pos = lax.broadcasted_iota(jnp.int32, (length, length), 0)
    col_pos = lax.broadcasted_iota(jnp.int32, (length, length), 1)
    allowed = (col_pos <= row_pos)[None, None] & (
        col_pos[None, None] < valid_lengths[:, :, None, None]
    )
    scores = jnp.where(allowed, scores, -jnp.inf)
    row_max = jnp.max(scores, axis=-1, keepdims=True)
    raised = jnp.where(allowed, jnp.exp(scores - row_max), 0.0)
    return (raised / jnp.sum(raised, axis=-1, keepdims=True)).astype(jnp.bfloat16)


def reduced(layer_inputs, saved_queries, saved_keys, held_weights, cotangent, valid_lengths):
    sections = lax.axis_size("section")
    position = lax.axis_index("section")
    inputs = layer_inputs[0]
    value_w = held_weights[0, :, 0]
    output_w = held_weights[0, :, 1]
    attend = attention_weights(saved_queries[0], saved_keys[0], valid_lengths)
    micro_count = inputs.shape[1]
    length = inputs.shape[2]
    model_width = inputs.shape[3]
    head_size = value_w.shape[2]
    values = jnp.einsum(
        "nmld,ndh->nmlh", inputs, value_w, preferred_element_type=jnp.float32
    ).astype(jnp.bfloat16)
    mixtures = jnp.einsum(
        "nmts,nmsh->nmth", attend, values, preferred_element_type=jnp.float32
    ).astype(jnp.bfloat16)
    is_end = [position == sections - 1, position == 0]
    starts = [sections - 1 - position, position]

    def make_compute(direction):

        def compute(operands):
            grads, uppers, vgrads, incoming, index = operands
            fresh = lax.dynamic_index_in_dim(cotangent[direction], index, 0, keepdims=False)
            upstream = jnp.where(is_end[direction], fresh, incoming)
            weights_now = lax.dynamic_index_in_dim(attend[direction], index, 0, keepdims=False)
            out_grad = jnp.dot(
                upstream, output_w[direction], preferred_element_type=jnp.float32
            ).astype(jnp.bfloat16)
            val_grad = jnp.einsum(
                "ts,th->sh", weights_now, out_grad, preferred_element_type=jnp.float32
            ).astype(jnp.bfloat16)
            branch = jnp.einsum(
                "lh,dh->ld", val_grad, value_w[direction], preferred_element_type=jnp.float32
            )
            grad_input = (upstream.astype(jnp.float32) + branch).astype(jnp.bfloat16)
            grads = lax.dynamic_update_index_in_dim(grads, grad_input, index, 0)
            uppers = lax.dynamic_update_index_in_dim(uppers, upstream, index, 0)
            vgrads = lax.dynamic_update_index_in_dim(vgrads, val_grad, index, 0)
            return (grad_input, (grads, uppers, vgrads))

        return compute

    def skip(operands):
        grads, uppers, vgrads, incoming, index = operands
        return (jnp.zeros_like(incoming), (grads, uppers, vgrads))

    def advance(moment, received, buffers):
        outgoing = []
        updated = []
        for direction in range(2):
            micro_id = moment - starts[direction]
            active = (micro_id >= 0) & (micro_id < micro_count)
            clipped = jnp.clip(micro_id, 0, micro_count - 1)
            grads, uppers, vgrads = buffers[direction]
            sent_now, fresh_buffers = lax.cond(
                active,
                make_compute(direction),
                skip,
                (grads, uppers, vgrads, received[direction], clipped),
            )
            outgoing.append(sent_now)
            updated.append(fresh_buffers)
        return (jnp.stack(outgoing), tuple(updated))

    big_zero = jnp.zeros((micro_count, length, model_width), jnp.bfloat16)
    small_zero = jnp.zeros((micro_count, length, head_size), jnp.bfloat16)
    buffers = ((big_zero, big_zero, small_zero), (big_zero, big_zero, small_zero))
    sent, buffers = advance(
        jnp.int32(0), jnp.zeros((2, length, model_width), jnp.bfloat16), buffers
    )

    def loop_body(moment, carried):
        outgoing, held = carried
        from_next = passed_along(outgoing[0], "section", -1)
        from_prev = passed_along(outgoing[1], "section", 1)
        return advance(moment, jnp.stack([from_next, from_prev]), held)

    sent, buffers = lax.fori_loop(1, sections + micro_count - 1, loop_body, (sent, buffers))
    grads_in = jnp.stack([buffers[0][0], buffers[1][0]])
    upstreams = jnp.stack([buffers[0][1], buffers[1][1]])
    val_grads = jnp.stack([buffers[0][2], buffers[1][2]])
    flat_in = inputs.reshape(2, micro_count * length, model_width)
    flat_up = upstreams.reshape(2, micro_count * length, model_width)
    flat_mix = mixtures.reshape(2, micro_count * length, head_size)
    flat_vg = val_grads.reshape(2, micro_count * length, head_size)
    grad_value = jnp.einsum("ntd,nth->dnh", flat_in, flat_vg, preferred_element_type=jnp.float32)
    grad_output = jnp.einsum("ntd,nth->dnh", flat_up, flat_mix, preferred_element_type=jnp.float32)
    summed = lax.psum_scatter(
        jnp.stack([grad_value, grad_output], axis=2).reshape(
            model_width // lax.axis_size("dp") * lax.axis_size("dp"), 4 * head_size
        ),
        "dp",
        scatter_dimension=0,
        tiled=True,
    )
    summed = summed.reshape(-1, 2, 2, head_size)
    own_part = summed[:, 0]
    mirror_part = summed[:, 1]
    for bit_no in range(sections.bit_length() - 1):
        mirror_part = from_partner(mirror_part.astype(jnp.bfloat16), "section", bit_no).astype(
            mirror_part.dtype
        )
    combined = own_part + mirror_part
    weight_grads = jnp.transpose(combined, (1, 0, 2))[None]
    return (grads_in[None], weight_grads)


def swapped(block, axis, mask):
    return lax.ppermute(block, axis, [(i, i ^ mask) for i in range(lax.axis_size(axis))])


def shifted(block, distance):
    count = lax.axis_size("dp")
    return lax.ppermute(block, "dp", [(i, (i + 2 * distance) % count) for i in range(count)])


def contract(left, right, left_dim, right_dim):
    return lax.dot_general(
        left, right, (((left_dim,), (right_dim,)), ((), ())), preferred_element_type=jnp.float32
    )


def block_attention(queries, key_vectors, valid_lengths):
    ways, seqs, length, head = queries.shape
    tokens = seqs * length
    scores = jnp.einsum(
        "nth,nsh->nts",
        queries.reshape(ways, tokens, head),
        key_vectors.reshape(ways, tokens, head),
        preferred_element_type=jnp.float32,
    ) / math.sqrt(head)
    row = lax.broadcasted_iota(jnp.int32, (tokens, tokens), 0)
    col = lax.broadcasted_iota(jnp.int32, (tokens, tokens), 1)
    bound = jnp.repeat(valid_lengths, length, axis=1)[:, None, :]
    allowed = ((row // length == col // length) & (col <= row))[None] & (
        (col % length)[None] < bound
    )
    scores = jnp.where(allowed, scores, -jnp.inf)
    row_max = jnp.max(scores, axis=-1, keepdims=True)
    raised = jnp.where(allowed, jnp.exp(scores - row_max), 0.0)
    return (raised / jnp.sum(raised, axis=-1, keepdims=True)).astype(jnp.bfloat16)


def chain_kernel(sections, tokens, head, place, *refs):
    parts = refs[:sections]
    gathered, steer, own = refs[sections:]
    products = (sections - 1) * head

    def at(here):
        mine = [[None] * sections, [None] * sections]
        for way in range(2):
            order = range(sections - 1, -1, -1) if way == 0 else range(sections)
            done = []
            for holder in order:
                part = parts[here ^ holder]
                first = products + way * tokens
                total = part[first : first + tokens, :].astype(jnp.float32)
                for other in done:
                    block = (other ^ holder) - 1
                    total += contract(
                        mine[way][other], part[block * head : (block + 1) * head, :], 1, 0
                    )
                base = products + 2 * tokens
                weights = part[base : base + tokens, way * tokens : (way + 1) * tokens]
                mine[way][holder] = contract(weights, total.astype(jnp.bfloat16), 0, 0).astype(
                    jnp.bfloat16
                )
                done.append(holder)
        zero = jnp.zeros((tokens, head), jnp.bfloat16)
        for far in range(sections):
            inside = here + far < sections
            gathered[0, far] = mine[0][here + far] if inside else zero
            gathered[1, far] = mine[1][sections - 1 - here - far] if inside else zero
        mirror = here ^ (sections - 1)
        base = products + 2 * tokens + tokens
        gathered[0, sections] = parts[0][base : base + tokens, :]
        gathered[1, sections] = parts[here ^ mirror][base + tokens : base + 2 * tokens, :]
        for way in range(2):
            own[way] = mine[way][here]
        for mask in range(1, sections):
            other = here ^ mask
            way = 0 if other > here else 1
            lanes = slice((mask - 1) * head, mask * head)
            steer[way * tokens : (way + 1) * tokens, lanes] = mine[way][other]
            steer[(1 - way) * tokens : (2 - way) * tokens, lanes] = zero

    for here in range(sections):

        @pl.when(place[0] == here)
        def _():
            at(here)


def input_kernel(sections, tokens, place, cot, steer, own, held, near, far, out):
    width = near.shape[2]
    core = place[1]
    for which, fetched in ((core, near), (1 - core, far)):
        start = pl.multiple_of(which * width, 128)
        sent = fetched[0, 0]
        total = contract(steer[:, : sent.shape[1]], sent, 1, 1)
        for mask in range(1, sections - 1):
            sent = fetched[mask, 0]
            head = sent.shape[1]
            total += contract(steer[:, mask * head : (mask + 1) * head], sent, 1, 1)
        for way in range(2):
            branch = contract(own[way], held[way, 0, pl.ds(start, width), :], 1, 1)
            branch += total[way * tokens : (way + 1) * tokens]
            base = cot[way, :, pl.ds(start, width)].astype(jnp.float32)
            out[way, :, pl.ds(start, width)] = (base + branch).astype(jnp.bfloat16)


def weight_kernel(sections, steps, *refs):
    columns = refs[:steps]
    near = refs[steps : 2 * steps]
    far, held, out = refs[2 * steps :]
    head = out.shape[-1]
    width = out.shape[1]
    for which in range(2):
        out[which] = jnp.zeros((width, head), jnp.float32)
    for step in range(steps):
        for side in range(2):
            for way in range(2):

                def sent(index):
                    return near[step][way, index] if side == 0 else far[step, way, index]

                inputs = columns[step][side, way]
                out[0] += contract(inputs, sent(0), 0, 0)
                upstream = columns[step][side, 2 + way].astype(jnp.float32)
                for index in range(1, sections):
                    upstream += contract(sent(index), held[way, index - 1], 1, 1)
                out[1] += contract(upstream.astype(jnp.bfloat16), sent(sections), 0, 0)


def gathered(layer_inputs, saved_queries, saved_keys, held_weights, cotangent, valid_lengths):
    sections = lax.axis_size("section")
    replicas = lax.axis_size("dp")
    steps = replicas // 2
    here = lax.axis_index("section")
    core = lax.axis_index("dp") % 2
    depth = lax.axis_index("dp") // 2
    inputs = layer_inputs[0]
    held = held_weights[0]
    seqs, length, model_width = inputs.shape[1:]
    tokens = seqs * length
    head = held.shape[-1]
    width = model_width // replicas
    inputs = inputs.reshape(2, tokens, model_width)
    cot = cotangent.reshape(2, tokens, model_width)
    halved = held.reshape(2, 2, steps, 2, width, head)

    fetched = []
    for mask in range(1, sections):
        way = jnp.where((here ^ mask) < here, 0, 1)
        piece = lax.dynamic_slice(
            halved, (way, 0, 0, core, 0, 0), (1, 1, steps, 1, width, head)
        ).reshape(steps, width, head)
        fetched.append(swapped(piece, "section", mask))

    mirrored = swapped(inputs[1], "section", sections - 1)
    own_slice = lax.dynamic_slice(
        halved, (1, 0, depth, core, 0, 0), (1, 1, 1, 1, width, head)
    ).reshape(width, head)
    lent = [own_slice]
    for mask in range(1, sections):
        route = [
            (i, i ^ mask) for i in range(sections) if i ^ mask < i < sections - 1 - (i ^ mask)
        ]
        lent.append(lax.ppermute(own_slice, "section", route) if route else None)

    attend = block_attention(saved_queries[0], saved_keys[0], valid_lengths)
    values = jnp.einsum(
        "ntd,ndh->nth", inputs, held[:, 0], preferred_element_type=jnp.float32
    ).astype(jnp.bfloat16)
    mixtures = jnp.einsum(
        "nts,nsh->nth", attend, values, preferred_element_type=jnp.float32
    ).astype(jnp.bfloat16)
    first_grad = jnp.einsum(
        "ntd,ndh->nth", cot, held[:, 1], preferred_element_type=jnp.float32
    ).astype(jnp.bfloat16)

    columns = jnp.stack([inputs[0], mirrored, cot[0], cot[1]])
    columns = columns.reshape(4, tokens, steps, 2, width)
    mine = lax.dynamic_index_in_dim(columns, core, 3, keepdims=False)
    other = lax.dynamic_index_in_dim(columns, 1 - core, 3, keepdims=False)
    both = jnp.stack([mine, swapped(other, "dp", 1)])
    pieces = []
    for distance in range(steps):
        piece = lax.dynamic_index_in_dim(both, (depth + distance) % steps, 3, keepdims=False)
        pieces.append(shifted(piece, distance) if distance else piece)

    products = []
    for mask in range(1, sections):
        way = jnp.where((here ^ mask) > here, 0, 1)
        output_half = lax.dynamic_slice(
            halved, (way, 1, 0, core, 0, 0), (1, 1, steps, 1, width, head)
        ).reshape(steps * width, head)
        products.append(contract(fetched[mask - 1].reshape(steps * width, head), output_half, 0, 0))
    products = jnp.stack(products)
    products = (products + swapped(products, "dp", 1)).astype(jnp.bfloat16)
    near = jnp.stack(fetched)
    far = swapped(near, "dp", 1)

    part = jnp.concatenate(
        [
            products.reshape(-1, head),
            first_grad.reshape(-1, head),
            jnp.pad(
                jnp.concatenate([attend[0], attend[1]], axis=1), ((0, 0), (0, head - 2 * tokens))
            ),
            mixtures.reshape(-1, head),
        ]
    )
    rows = part.shape[0] - 2 * tokens
    parts = [part]
    for mask in range(1, sections):
        parts.append(swapped(part if mask == sections - 1 else part[:rows], "section", mask))

    place = jnp.stack([here, core])
    memory = pl.BlockSpec(memory_space=pltpu.VMEM)
    scalars = pl.BlockSpec(memory_space=pltpu.SMEM)
    sent, steer, own = pl.pallas_call(
        functools.partial(chain_kernel, sections, tokens, head),
        in_specs=[scalars] + [memory] * sections,
        out_specs=(memory, memory, memory),
        out_shape=(
            jax.ShapeDtypeStruct((2, sections + 1, tokens, head), jnp.bfloat16),
            jax.ShapeDtypeStruct((2 * tokens, (sections - 1) * head), jnp.bfloat16),
            jax.ShapeDtypeStruct((2, tokens, head), jnp.bfloat16),
        ),
        name="chain",
    )(place, *parts)

    near_sent = [shifted(sent, distance) if distance else sent for distance in range(steps)]
    far_sent = swapped(jnp.stack(near_sent), "dp", 1)

    grads_in = pl.pallas_call(
        functools.partial(input_kernel, sections, tokens),
        grid=(steps,),
        in_specs=[
            scalars,
            pl.BlockSpec((2, tokens, 2 * width), lambda i: (0, 0, i)),
            pl.BlockSpec((2 * tokens, (sections - 1) * head), lambda i: (0, 0)),
            pl.BlockSpec((2, tokens, head), lambda i: (0, 0, 0)),
            pl.BlockSpec((2, 1, 2 * width, head), lambda i: (0, 0, i, 0)),
            pl.BlockSpec((sections - 1, 1, width, head), lambda i: (0, i, 0, 0)),
            pl.BlockSpec((sections - 1, 1, width, head), lambda i: (0, i, 0, 0)),
        ],
        out_specs=pl.BlockSpec((2, tokens, 2 * width), lambda i: (0, 0, i)),
        out_shape=jax.ShapeDtypeStruct((2, tokens, model_width), jnp.bfloat16),
        name="input_side",
    )(place, cot, steer, own, held, near, far)

    sliced = [own_slice] + [
        lax.dynamic_index_in_dim(block, depth, 0, keepdims=False) for block in fetched
    ]
    down = jnp.stack(sliced)
    up = jnp.stack(
        [own_slice]
        + [
            sliced[mask]
            if lent[mask] is None
            else jnp.where((here ^ mask) < here, sliced[mask], lent[mask])
            for mask in range(1, sections)
        ]
    )
    nearby = []
    for distance in range(1, sections):
        inside = here + distance < sections
        below = jnp.where(inside, here ^ (here + distance), 0)
        above = jnp.where(inside, here ^ (sections - 1 - here - distance), 0)
        nearby.append(
            jnp.stack(
                [
                    lax.dynamic_index_in_dim(down, below, 0, keepdims=False),
                    lax.dynamic_index_in_dim(up, above, 0, keepdims=False),
                ]
            )
        )
    nearby = jnp.stack(nearby, axis=1)

    weight_grads = pl.pallas_call(
        functools.partial(weight_kernel, sections, steps),
        in_specs=[memory] * (2 * steps + 2),
        out_specs=memory,
        out_shape=jax.ShapeDtypeStruct((2, width, head), jnp.float32),
        name="weight_side",
    )(*pieces, *near_sent, far_sent, nearby)
    shape = (1, 2, seqs, length, model_width)
    return (grads_in.reshape(shape), weight_grads[None])


def shards(*operands):
    layer_inputs, held_weights = operands[0], operands[3]
    sections = lax.axis_size("section")
    replicas = lax.axis_size("dp")
    seqs, length, model_width = layer_inputs.shape[2:]
    head = held_weights.shape[-1]
    every_token = replicas * seqs * length
    moved = 2 * every_token * ((sections + 1) * head + 2 * model_width // replicas) * 2
    partial_sums = 4 * model_width * head * 4
    even = replicas % 2 == 0 and sections > 1 and sections & (sections - 1) == 0
    if even and moved < partial_sums and 2 * seqs * length <= head:
        return gathered(*operands)
    return reduced(*operands)


def solution(mesh):
    return jax.shard_map(
        shards,
        mesh=mesh,
        in_specs=(
            P("section", None, "dp", None, None),
            P("section", None, "dp", None, None),
            P("section", None, "dp", None, None),
            P("section", None, None, None, None),
            P(None, "dp", None, None),
            P(None, "dp"),
        ),
        out_specs=(P("section", None, "dp", None, None), P("section", None, "dp", None)),
        check_vma=False,
    )
```

```python
import functools
import math

import jax
import jax.numpy as jnp
from jax import lax
from jax.experimental import pallas as pl
from jax.experimental.pallas import tpu as pltpu
from jax.sharding import PartitionSpec as P


def passed_along(block, axis, distance):
    devices = range(lax.axis_size(axis))
    route = [(i - distance, i) for i in devices if i - distance in devices]
    return lax.ppermute(block, axis, route)


def from_partner(block, axis, bit):
    count = lax.axis_size(axis)
    route = []
    for low in range(count):
        high = low | 1 << bit
        if high != low and high < count:
            route += [(low, high), (high, low)]
    return lax.ppermute(block, axis, route)


def attention_weights(queries, key_vectors, valid_lengths):
    length = queries.shape[-2]
    scores = jnp.einsum(
        "nmth,nmsh->nmts", queries, key_vectors, preferred_element_type=jnp.float32
    ) / math.sqrt(queries.shape[-1])
    row_pos = lax.broadcasted_iota(jnp.int32, (length, length), 0)
    col_pos = lax.broadcasted_iota(jnp.int32, (length, length), 1)
    allowed = (col_pos <= row_pos)[None, None] & (
        col_pos[None, None] < valid_lengths[:, :, None, None]
    )
    scores = jnp.where(allowed, scores, -jnp.inf)
    row_max = jnp.max(scores, axis=-1, keepdims=True)
    raised = jnp.where(allowed, jnp.exp(scores - row_max), 0.0)
    return (raised / jnp.sum(raised, axis=-1, keepdims=True)).astype(jnp.bfloat16)


def reduced(layer_inputs, saved_queries, saved_keys, held_weights, cotangent, valid_lengths):
    sections = lax.axis_size("section")
    position = lax.axis_index("section")
    inputs = layer_inputs[0]
    value_w = held_weights[0, :, 0]
    output_w = held_weights[0, :, 1]
    attend = attention_weights(saved_queries[0], saved_keys[0], valid_lengths)
    micro_count = inputs.shape[1]
    length = inputs.shape[2]
    model_width = inputs.shape[3]
    head_size = value_w.shape[2]
    values = jnp.einsum(
        "nmld,ndh->nmlh", inputs, value_w, preferred_element_type=jnp.float32
    ).astype(jnp.bfloat16)
    mixtures = jnp.einsum(
        "nmts,nmsh->nmth", attend, values, preferred_element_type=jnp.float32
    ).astype(jnp.bfloat16)
    is_end = [position == sections - 1, position == 0]
    starts = [sections - 1 - position, position]

    def make_compute(direction):

        def compute(operands):
            grads, uppers, vgrads, incoming, index = operands
            fresh = lax.dynamic_index_in_dim(cotangent[direction], index, 0, keepdims=False)
            upstream = jnp.where(is_end[direction], fresh, incoming)
            weights_now = lax.dynamic_index_in_dim(attend[direction], index, 0, keepdims=False)
            out_grad = jnp.dot(
                upstream, output_w[direction], preferred_element_type=jnp.float32
            ).astype(jnp.bfloat16)
            val_grad = jnp.einsum(
                "ts,th->sh", weights_now, out_grad, preferred_element_type=jnp.float32
            ).astype(jnp.bfloat16)
            branch = jnp.einsum(
                "lh,dh->ld", val_grad, value_w[direction], preferred_element_type=jnp.float32
            )
            grad_input = (upstream.astype(jnp.float32) + branch).astype(jnp.bfloat16)
            grads = lax.dynamic_update_index_in_dim(grads, grad_input, index, 0)
            uppers = lax.dynamic_update_index_in_dim(uppers, upstream, index, 0)
            vgrads = lax.dynamic_update_index_in_dim(vgrads, val_grad, index, 0)
            return (grad_input, (grads, uppers, vgrads))

        return compute

    def skip(operands):
        grads, uppers, vgrads, incoming, _ = operands
        return (jnp.zeros_like(incoming), (grads, uppers, vgrads))

    def advance(moment, received, buffers):
        outgoing = []
        updated = []
        for direction in range(2):
            micro_id = moment - starts[direction]
            active = (micro_id >= 0) & (micro_id < micro_count)
            clipped = jnp.clip(micro_id, 0, micro_count - 1)
            grads, uppers, vgrads = buffers[direction]
            sent_now, fresh_buffers = lax.cond(
                active,
                make_compute(direction),
                skip,
                (grads, uppers, vgrads, received[direction], clipped),
            )
            outgoing.append(sent_now)
            updated.append(fresh_buffers)
        return (jnp.stack(outgoing), tuple(updated))

    big_zero = jnp.zeros((micro_count, length, model_width), jnp.bfloat16)
    small_zero = jnp.zeros((micro_count, length, head_size), jnp.bfloat16)
    buffers = ((big_zero, big_zero, small_zero), (big_zero, big_zero, small_zero))
    sent, buffers = advance(
        jnp.int32(0), jnp.zeros((2, length, model_width), jnp.bfloat16), buffers
    )

    def loop_body(moment, carried):
        outgoing, held = carried
        from_next = passed_along(outgoing[0], "section", -1)
        from_prev = passed_along(outgoing[1], "section", 1)
        return advance(moment, jnp.stack([from_next, from_prev]), held)

    sent, buffers = lax.fori_loop(1, sections + micro_count - 1, loop_body, (sent, buffers))
    grads_in = jnp.stack([buffers[0][0], buffers[1][0]])
    upstreams = jnp.stack([buffers[0][1], buffers[1][1]])
    val_grads = jnp.stack([buffers[0][2], buffers[1][2]])
    flat_in = inputs.reshape(2, micro_count * length, model_width)
    flat_up = upstreams.reshape(2, micro_count * length, model_width)
    flat_mix = mixtures.reshape(2, micro_count * length, head_size)
    flat_vg = val_grads.reshape(2, micro_count * length, head_size)
    grad_value = jnp.einsum("ntd,nth->dnh", flat_in, flat_vg, preferred_element_type=jnp.float32)
    grad_output = jnp.einsum("ntd,nth->dnh", flat_up, flat_mix, preferred_element_type=jnp.float32)
    summed = lax.psum_scatter(
        jnp.stack([grad_value, grad_output], axis=2).reshape(
            model_width // lax.axis_size("dp") * lax.axis_size("dp"), 4 * head_size
        ),
        "dp",
        scatter_dimension=0,
        tiled=True,
    )
    summed = summed.reshape(-1, 2, 2, head_size)
    own_part = summed[:, 0]
    mirror_part = summed[:, 1]
    for bit_no in range(sections.bit_length() - 1):
        mirror_part = from_partner(mirror_part.astype(jnp.bfloat16), "section", bit_no).astype(
            mirror_part.dtype
        )
    combined = own_part + mirror_part
    weight_grads = jnp.transpose(combined, (1, 0, 2))[None]
    return (grads_in[None], weight_grads)


def swapped(block, axis, mask):
    return lax.ppermute(block, axis, [(i, i ^ mask) for i in range(lax.axis_size(axis))])


def shifted(block, distance):
    count = lax.axis_size("dp")
    return lax.ppermute(block, "dp", [(i, (i + 2 * distance) % count) for i in range(count)])


def contract(left, right, left_dim, right_dim):
    return lax.dot_general(
        left, right, (((left_dim,), (right_dim,)), ((), ())), preferred_element_type=jnp.float32
    )


def block_attention(queries, key_vectors, valid_lengths):
    ways, seqs, length, head = queries.shape
    tokens = seqs * length
    scores = jnp.einsum(
        "nth,nsh->nts",
        queries.reshape(ways, tokens, head),
        key_vectors.reshape(ways, tokens, head),
        preferred_element_type=jnp.float32,
    ) / math.sqrt(head)
    row = lax.broadcasted_iota(jnp.int32, (tokens, tokens), 0)
    col = lax.broadcasted_iota(jnp.int32, (tokens, tokens), 1)
    bound = jnp.repeat(valid_lengths, length, axis=1)[:, None, :]
    allowed = ((row // length == col // length) & (col <= row))[None] & (
        (col % length)[None] < bound
    )
    scores = jnp.where(allowed, scores, -jnp.inf)
    row_max = jnp.max(scores, axis=-1, keepdims=True)
    raised = jnp.where(allowed, jnp.exp(scores - row_max), 0.0)
    return (raised / jnp.sum(raised, axis=-1, keepdims=True)).astype(jnp.bfloat16)


def chain_kernel(sections, tokens, head, place, *refs):
    parts = refs[:sections]
    gathered, steer, own = refs[sections:]
    products = (sections - 1) * head

    def at(here):
        mine = [[None] * sections, [None] * sections]
        for way in range(2):
            order = range(sections - 1, -1, -1) if way == 0 else range(sections)
            done = []
            for holder in order:
                part = parts[here ^ holder]
                first = products + way * tokens
                total = part[first : first + tokens, :].astype(jnp.float32)
                for other in done:
                    block = (other ^ holder) - 1
                    total += contract(
                        mine[way][other], part[block * head : (block + 1) * head, :], 1, 0
                    )
                base = products + 2 * tokens
                weights = part[base : base + tokens, way * tokens : (way + 1) * tokens]
                mine[way][holder] = contract(weights, total.astype(jnp.bfloat16), 0, 0).astype(
                    jnp.bfloat16
                )
                done.append(holder)
        zero = jnp.zeros((tokens, head), jnp.bfloat16)
        for far in range(sections):
            inside = here + far < sections
            gathered[0, far] = mine[0][here + far] if inside else zero
            gathered[1, far] = mine[1][sections - 1 - here - far] if inside else zero
        mirror = here ^ (sections - 1)
        base = products + 2 * tokens + tokens
        gathered[0, sections] = parts[0][base : base + tokens, :]
        gathered[1, sections] = parts[here ^ mirror][base + tokens : base + 2 * tokens, :]
        for way in range(2):
            own[way] = mine[way][here]
        for mask in range(1, sections):
            other = here ^ mask
            way = 0 if other > here else 1
            lanes = slice((mask - 1) * head, mask * head)
            steer[way * tokens : (way + 1) * tokens, lanes] = mine[way][other]
            steer[(1 - way) * tokens : (2 - way) * tokens, lanes] = zero

    for here in range(sections):

        @pl.when(place[0] == here)
        def _():
            at(here)


def input_kernel(sections, tokens, place, cot, steer, own, held, *refs):
    near, far = refs[: sections - 1], refs[sections - 1 : 2 * sections - 2]
    out = refs[2 * sections - 2]
    width = near[0].shape[1]
    core = place[1]
    for which, fetched in ((core, near), (1 - core, far)):
        start = pl.multiple_of(which * width, 128)
        weights = jnp.concatenate([block[0] for block in fetched], axis=1)
        total = contract(steer[...], weights, 1, 1)
        for way in range(2):
            branch = contract(own[way], held[way, 0, pl.ds(start, width), :], 1, 1)
            branch += total[way * tokens : (way + 1) * tokens]
            base = cot[way, :, pl.ds(start, width)].astype(jnp.float32)
            out[way, :, pl.ds(start, width)] = (base + branch).astype(jnp.bfloat16)


def pick_weights(sections, place, halved, *refs):
    outs, sems = refs[: sections - 1], refs[sections - 1]
    here, core = place[0], place[1]
    copies = []
    for mask in range(sections - 1, 0, -1):
        way = jnp.where((here ^ mask) < here, 0, 1)
        copy = pltpu.make_async_copy(
            halved.at[way, 0, :, core], outs[mask - 1], sems.at[mask - 1]
        )
        copy.start()
        copies.append(copy)
    for copy in copies:
        copy.wait()


def carried_out(copies):
    for copy in copies:
        copy.start()
    for copy in copies:
        copy.wait()


def pick_outputs(place, halved, out, sem):
    carried_out([pltpu.make_async_copy(halved.at[:, 1, :, place[1]], out, sem)])


def pick_columns(steps, width, place, inputs, cot, *refs):
    outs, sems = refs[:steps], refs[steps]
    copies = []
    for distance in range(steps):
        start = pl.multiple_of((place[2] + distance) % steps * 2 * width, 128)
        copies.append(
            pltpu.make_async_copy(
                inputs.at[:, :, pl.ds(start, 2 * width)],
                outs[distance].at[0:2],
                sems.at[3 * distance],
            )
        )
        for way in range(2):
            half = pl.multiple_of(start + place[3 + way] * width, 128)
            copies.append(
                pltpu.make_async_copy(
                    cot.at[way, :, pl.ds(half, width)],
                    outs[distance].at[2, :, way * width : (way + 1) * width],
                    sems.at[3 * distance + 1 + way],
                )
            )
    carried_out(copies)


def pick_moving(steps, *refs):
    sources, upward, sems = refs[:steps], refs[steps], refs[steps + 3]
    width = upward.shape[-1] // 2
    copies = []
    for step, source in enumerate(sources):
        copies.append(pltpu.make_async_copy(source.at[1], upward.at[step], sems.at[3 * step]))
        for way in range(2):
            half = source.at[2, :, way * width : (way + 1) * width]
            copies.append(
                pltpu.make_async_copy(
                    half, refs[steps + 1 + way].at[step], sems.at[3 * step + 1 + way]
                )
            )
    carried_out(copies)


def product_kernel(sections, steps, place, outputs, *refs):
    fetched, out = refs[: sections - 1], refs[sections - 1]
    for mask in range(1, sections):
        way = jnp.where((place[0] ^ mask) > place[0], 0, 1)
        total = None
        for step in range(steps):
            term = contract(fetched[mask - 1][step], outputs[way, step], 0, 0)
            total = term if total is None else total + term
        out[mask - 1] = total


def weight_kernel(sections, steps, tokens, place, *refs):
    columns = refs[: 2 * steps]
    mirrored, lent = refs[2 * steps : 2 * steps + 2], refs[2 * steps + 2 : 2 * steps + 6]
    sent = refs[2 * steps + 6 : 4 * steps + 6]
    held, out, lefts, rights, steers = refs[4 * steps + 6 :]
    width, head = out.shape[1:]
    every = 2 * steps * tokens
    lanes = pl.ds(pl.multiple_of(place[1] * width, 128), width)
    for index in range(2 * steps):
        rows = slice(index * tokens, (index + 1) * tokens)
        for way in range(2):
            for far in range(1, sections):
                steers[way, rows, (far - 1) * head : far * head] = sent[index][way, far]
            both = slice(way * every + index * tokens, way * every + (index + 1) * tokens)
            lefts[0, both, :] = sent[index][way, 0]
            lefts[1, both, :] = sent[index][way, sections]
        rights[rows, :] = columns[index][0, :, lanes]
        rows = slice(every + index * tokens, every + (index + 1) * tokens)
        rights[rows, :] = mirrored[index // steps][index % steps, :, lanes]
    out[0] = contract(lefts[0], rights[...], 0, 0).T
    for index in range(2 * steps):
        for way in range(2):
            both = slice(way * every + index * tokens, way * every + (index + 1) * tokens)
            half = slice(way * width, (way + 1) * width)

            @pl.when(place[3 + way] == place[1])
            def _():
                rights[both, :] = columns[index][2, :, half]

            @pl.when(place[3 + way] != place[1])
            def _():
                rights[both, :] = lent[2 * (index // steps) + way][index % steps]

    for way in range(2):
        rows = slice(way * every, (way + 1) * every)
        total = contract(steers[way], held[way], 1, 1)
        rights[rows, :] = (rights[rows, :].astype(jnp.float32) + total).astype(jnp.bfloat16)
    out[1] = contract(lefts[1], rights[...], 0, 0).T


def gathered(layer_inputs, saved_queries, saved_keys, held_weights, cotangent, valid_lengths):
    sections = lax.axis_size("section")
    replicas = lax.axis_size("dp")
    steps = replicas // 2
    here = lax.axis_index("section")
    core = lax.axis_index("dp") % 2
    depth = lax.axis_index("dp") // 2
    inputs = layer_inputs[0]
    held = held_weights[0]
    seqs, length, model_width = inputs.shape[1:]
    tokens = seqs * length
    head = held.shape[-1]
    width = model_width // replicas
    inputs = inputs.reshape(2, tokens, model_width)
    cot = cotangent.reshape(2, tokens, model_width)
    halved = held.reshape(2, 2, steps, 2, width, head)
    asides = (sections // 2, 1)
    place = jnp.stack([here, core, depth] + [jnp.where(here & aside, 1, 0) for aside in asides])
    memory = pl.BlockSpec(memory_space=pltpu.VMEM)
    scalars = pl.BlockSpec(memory_space=pltpu.SMEM)
    anywhere = pl.BlockSpec(memory_space=pl.ANY)
    hbm = pl.BlockSpec(memory_space=pltpu.HBM)

    picked = pl.pallas_call(
        functools.partial(pick_weights, sections),
        in_specs=[scalars, hbm],
        out_specs=[memory] * (sections - 1),
        out_shape=[jax.ShapeDtypeStruct((steps, width, head), jnp.bfloat16)] * (sections - 1),
        scratch_shapes=[pltpu.SemaphoreType.DMA((sections - 1,))],
        name="pick_weights",
        compiler_params=pltpu.CompilerParams(vmem_limit_bytes=61 << 20),
    )(place, halved)
    fetched = [None] * sections
    for mask in range(sections - 1, 0, -1):
        fetched[mask] = swapped(picked[mask - 1], "section", mask)

    picked = pl.pallas_call(
        functools.partial(pick_columns, steps, width),
        in_specs=[scalars] + [hbm] * 2,
        out_specs=[memory] * steps,
        out_shape=[jax.ShapeDtypeStruct((3, tokens, 2 * width), jnp.bfloat16)] * steps,
        scratch_shapes=[pltpu.SemaphoreType.DMA((3 * steps,))],
        name="pick_columns",
        compiler_params=pltpu.CompilerParams(vmem_limit_bytes=8 << 20),
    )(place, inputs, cot)
    near_columns = [picked[0]]
    for distance in range(1, steps):
        near_columns.append(shifted(picked[distance], distance))

    attend = block_attention(saved_queries[0], saved_keys[0], valid_lengths)
    values = jnp.einsum(
        "ntd,ndh->nth", inputs, held[:, 0], preferred_element_type=jnp.float32
    ).astype(jnp.bfloat16)
    mixtures = jnp.einsum(
        "nts,nsh->nth", attend, values, preferred_element_type=jnp.float32
    ).astype(jnp.bfloat16)
    first_grad = jnp.einsum(
        "ntd,ndh->nth", cot, held[:, 1], preferred_element_type=jnp.float32
    ).astype(jnp.bfloat16)

    outputs = pl.pallas_call(
        pick_outputs,
        in_specs=[scalars, hbm],
        out_specs=memory,
        out_shape=jax.ShapeDtypeStruct((2, steps, width, head), jnp.bfloat16),
        scratch_shapes=[pltpu.SemaphoreType.DMA],
        name="pick_outputs",
        compiler_params=pltpu.CompilerParams(vmem_limit_bytes=58 << 20),
    )(place, halved)
    products = pl.pallas_call(
        functools.partial(product_kernel, sections, steps),
        in_specs=[scalars] + [memory] * sections,
        out_specs=memory,
        out_shape=jax.ShapeDtypeStruct((sections - 1, head, head), jnp.float32),
        name="products",
        compiler_params=pltpu.CompilerParams(vmem_limit_bytes=8 << 20),
    )(place, outputs, *fetched[1:])
    products = (products + swapped(products, "dp", 1)).astype(jnp.bfloat16)
    lent_back = [None] * sections
    for mask in range(1, sections):
        lent_back[mask] = swapped(fetched[mask], "dp", 1)

    part = jnp.concatenate(
        [
            products.reshape(-1, head),
            first_grad.reshape(-1, head),
            jnp.pad(
                jnp.concatenate([attend[0], attend[1]], axis=1), ((0, 0), (0, head - 2 * tokens))
            ),
            mixtures.reshape(-1, head),
        ]
    )
    rows = part.shape[0] - 2 * tokens
    parts = [part]
    for mask in range(1, sections):
        parts.append(swapped(part if mask == sections - 1 else part[:rows], "section", mask))

    upward, *sideways = pl.pallas_call(
        functools.partial(pick_moving, steps),
        in_specs=[anywhere] * steps,
        out_specs=[memory] * 3,
        out_shape=[jax.ShapeDtypeStruct((steps, tokens, 2 * width), jnp.bfloat16)]
        + [jax.ShapeDtypeStruct((steps, tokens, width), jnp.bfloat16)] * 2,
        scratch_shapes=[pltpu.SemaphoreType.DMA((3 * steps,))],
        name="pick_moving",
        compiler_params=pltpu.CompilerParams(vmem_limit_bytes=8 << 20),
    )(*near_columns)
    near_mirror = swapped(upward, "section", sections - 1)
    near_aside, far_aside = [], []
    for way in range(2):
        near_aside.append(swapped(sideways[way], "section", asides[way]))
    far_mirror = swapped(near_mirror, "dp", 1)
    for way in range(2):
        far_aside.append(swapped(near_aside[way], "dp", 1))
    far_columns = []
    for distance in range(steps):
        far_columns.append(swapped(near_columns[distance], "dp", 1))
    own_slice = lax.dynamic_slice(
        halved, (1, 0, depth, core, 0, 0), (1, 1, 1, 1, width, head)
    ).reshape(width, head)
    lent = [own_slice]
    for mask in range(1, sections):
        route = [
            (i, i ^ mask) for i in range(sections) if i ^ mask < i < sections - 1 - (i ^ mask)
        ]
        lent.append(lax.ppermute(own_slice, "section", route) if route else None)

    sent, steer, own = pl.pallas_call(
        functools.partial(chain_kernel, sections, tokens, head),
        in_specs=[scalars] + [memory] * sections,
        out_specs=(memory, memory, memory),
        out_shape=(
            jax.ShapeDtypeStruct((2, sections + 1, tokens, head), jnp.bfloat16),
            jax.ShapeDtypeStruct((2 * tokens, (sections - 1) * head), jnp.bfloat16),
            jax.ShapeDtypeStruct((2, tokens, head), jnp.bfloat16),
        ),
        name="chain",
        compiler_params=pltpu.CompilerParams(vmem_limit_bytes=8 << 20),
    )(place, *parts)

    near_sent = [sent]
    for distance in range(1, steps):
        near_sent.append(shifted(sent, distance))
    far_sent = []
    for distance in range(steps):
        far_sent.append(swapped(near_sent[distance], "dp", 1))

    grads_in = pl.pallas_call(
        functools.partial(input_kernel, sections, tokens),
        grid=(steps,),
        in_specs=[
            scalars,
            pl.BlockSpec((2, tokens, 2 * width), lambda i: (0, 0, i)),
            pl.BlockSpec((2 * tokens, (sections - 1) * head), lambda i: (0, 0)),
            pl.BlockSpec((2, tokens, head), lambda i: (0, 0, 0)),
            pl.BlockSpec((2, 1, 2 * width, head), lambda i: (0, 0, i, 0)),
        ]
        + [pl.BlockSpec((1, width, head), lambda i: (i, 0, 0))] * (2 * sections - 2),
        out_specs=pl.BlockSpec((2, tokens, 2 * width), lambda i: (0, 0, i)),
        out_shape=jax.ShapeDtypeStruct((2, tokens, model_width), jnp.bfloat16),
        name="input_side",
        compiler_params=pltpu.CompilerParams(vmem_limit_bytes=61 << 20),
    )(place, cot, steer, own, held, *fetched[1:], *lent_back[1:])

    sliced = [own_slice] + [
        lax.dynamic_index_in_dim(block, depth, 0, keepdims=False) for block in fetched[1:]
    ]
    down = jnp.stack(sliced)
    up = jnp.stack(
        [own_slice]
        + [
            sliced[mask]
            if lent[mask] is None
            else jnp.where((here ^ mask) < here, sliced[mask], lent[mask])
            for mask in range(1, sections)
        ]
    )
    nearby = []
    for distance in range(1, sections):
        inside = here + distance < sections
        below = jnp.where(inside, here ^ (here + distance), 0)
        above = jnp.where(inside, here ^ (sections - 1 - here - distance), 0)
        nearby.append(
            jnp.stack(
                [
                    lax.dynamic_index_in_dim(down, below, 0, keepdims=False),
                    lax.dynamic_index_in_dim(up, above, 0, keepdims=False),
                ]
            )
        )
    nearby = jnp.concatenate(nearby, axis=2)

    every = replicas * tokens
    weight_grads = pl.pallas_call(
        functools.partial(weight_kernel, sections, steps, tokens),
        in_specs=[scalars] + [memory] * (4 * steps + 7),
        out_specs=memory,
        out_shape=jax.ShapeDtypeStruct((2, width, head), jnp.float32),
        scratch_shapes=[
            pltpu.VMEM((2, 2 * every, head), jnp.bfloat16),
            pltpu.VMEM((2 * every, width), jnp.bfloat16),
            pltpu.VMEM((2, every, (sections - 1) * head), jnp.bfloat16),
        ],
        name="weight_side",
        compiler_params=pltpu.CompilerParams(vmem_limit_bytes=20 << 20),
    )(
        place,
        *near_columns,
        *far_columns,
        near_mirror,
        far_mirror,
        *near_aside,
        *far_aside,
        *near_sent,
        *far_sent,
        nearby,
    )
    shape = (1, 2, seqs, length, model_width)
    return (grads_in.reshape(shape), weight_grads[None])


def shards(*operands):
    layer_inputs, held_weights = operands[0], operands[3]
    sections = lax.axis_size("section")
    replicas = lax.axis_size("dp")
    seqs, length, model_width = layer_inputs.shape[2:]
    head = held_weights.shape[-1]
    every_token = replicas * seqs * length
    moved = 2 * every_token * ((sections + 1) * head + 2 * model_width // replicas) * 2
    partial_sums = 4 * model_width * head * 4
    even = replicas % 2 == 0 and sections > 1 and sections & (sections - 1) == 0
    if even and moved < partial_sums and 2 * seqs * length <= head:
        return gathered(*operands)
    return reduced(*operands)


def solution(mesh):
    return jax.shard_map(
        shards,
        mesh=mesh,
        in_specs=(
            P("section", None, "dp", None, None),
            P("section", None, "dp", None, None),
            P("section", None, "dp", None, None),
            P("section", None, None, None, None),
            P(None, "dp", None, None),
            P(None, "dp"),
        ),
        out_specs=(P("section", None, "dp", None, None), P("section", None, "dp", None)),
        check_vma=False,
    )
```

```python
import functools
import math

import jax
import jax.numpy as jnp
from jax import lax
from jax.experimental import pallas as pl
from jax.experimental.pallas import tpu as pltpu
from jax.sharding import PartitionSpec as P


def passed_along(block, axis, distance):
    devices = range(lax.axis_size(axis))
    route = [(i - distance, i) for i in devices if i - distance in devices]
    return lax.ppermute(block, axis, route)


def from_partner(block, axis, bit):
    count = lax.axis_size(axis)
    route = []
    for low in range(count):
        high = low | 1 << bit
        if high != low and high < count:
            route += [(low, high), (high, low)]
    return lax.ppermute(block, axis, route)


def attention_weights(queries, key_vectors, valid_lengths):
    length = queries.shape[-2]
    scores = jnp.einsum(
        "nmth,nmsh->nmts", queries, key_vectors, preferred_element_type=jnp.float32
    ) / math.sqrt(queries.shape[-1])
    row_pos = lax.broadcasted_iota(jnp.int32, (length, length), 0)
    col_pos = lax.broadcasted_iota(jnp.int32, (length, length), 1)
    allowed = (col_pos <= row_pos)[None, None] & (
        col_pos[None, None] < valid_lengths[:, :, None, None]
    )
    scores = jnp.where(allowed, scores, -jnp.inf)
    row_max = jnp.max(scores, axis=-1, keepdims=True)
    raised = jnp.where(allowed, jnp.exp(scores - row_max), 0.0)
    return (raised / jnp.sum(raised, axis=-1, keepdims=True)).astype(jnp.bfloat16)


def reduced(layer_inputs, saved_queries, saved_keys, held_weights, cotangent, valid_lengths):
    sections = lax.axis_size("section")
    position = lax.axis_index("section")
    inputs = layer_inputs[0]
    value_w = held_weights[0, :, 0]
    output_w = held_weights[0, :, 1]
    attend = attention_weights(saved_queries[0], saved_keys[0], valid_lengths)
    micro_count = inputs.shape[1]
    length = inputs.shape[2]
    model_width = inputs.shape[3]
    head_size = value_w.shape[2]
    values = jnp.einsum(
        "nmld,ndh->nmlh", inputs, value_w, preferred_element_type=jnp.float32
    ).astype(jnp.bfloat16)
    mixtures = jnp.einsum(
        "nmts,nmsh->nmth", attend, values, preferred_element_type=jnp.float32
    ).astype(jnp.bfloat16)
    is_end = [position == sections - 1, position == 0]
    starts = [sections - 1 - position, position]

    def make_compute(direction):

        def compute(operands):
            grads, uppers, vgrads, incoming, index = operands
            fresh = lax.dynamic_index_in_dim(cotangent[direction], index, 0, keepdims=False)
            upstream = jnp.where(is_end[direction], fresh, incoming)
            weights_now = lax.dynamic_index_in_dim(attend[direction], index, 0, keepdims=False)
            out_grad = jnp.dot(
                upstream, output_w[direction], preferred_element_type=jnp.float32
            ).astype(jnp.bfloat16)
            val_grad = jnp.einsum(
                "ts,th->sh", weights_now, out_grad, preferred_element_type=jnp.float32
            ).astype(jnp.bfloat16)
            branch = jnp.einsum(
                "lh,dh->ld", val_grad, value_w[direction], preferred_element_type=jnp.float32
            )
            grad_input = (upstream.astype(jnp.float32) + branch).astype(jnp.bfloat16)
            grads = lax.dynamic_update_index_in_dim(grads, grad_input, index, 0)
            uppers = lax.dynamic_update_index_in_dim(uppers, upstream, index, 0)
            vgrads = lax.dynamic_update_index_in_dim(vgrads, val_grad, index, 0)
            return (grad_input, (grads, uppers, vgrads))

        return compute

    def skip(operands):
        grads, uppers, vgrads, incoming, _ = operands
        return (jnp.zeros_like(incoming), (grads, uppers, vgrads))

    def advance(moment, received, buffers):
        outgoing = []
        updated = []
        for direction in range(2):
            micro_id = moment - starts[direction]
            active = (micro_id >= 0) & (micro_id < micro_count)
            clipped = jnp.clip(micro_id, 0, micro_count - 1)
            grads, uppers, vgrads = buffers[direction]
            sent_now, fresh_buffers = lax.cond(
                active,
                make_compute(direction),
                skip,
                (grads, uppers, vgrads, received[direction], clipped),
            )
            outgoing.append(sent_now)
            updated.append(fresh_buffers)
        return (jnp.stack(outgoing), tuple(updated))

    big_zero = jnp.zeros((micro_count, length, model_width), jnp.bfloat16)
    small_zero = jnp.zeros((micro_count, length, head_size), jnp.bfloat16)
    buffers = ((big_zero, big_zero, small_zero), (big_zero, big_zero, small_zero))
    sent, buffers = advance(
        jnp.int32(0), jnp.zeros((2, length, model_width), jnp.bfloat16), buffers
    )

    def loop_body(moment, carried):
        outgoing, held = carried
        from_next = passed_along(outgoing[0], "section", -1)
        from_prev = passed_along(outgoing[1], "section", 1)
        return advance(moment, jnp.stack([from_next, from_prev]), held)

    sent, buffers = lax.fori_loop(1, sections + micro_count - 1, loop_body, (sent, buffers))
    grads_in = jnp.stack([buffers[0][0], buffers[1][0]])
    upstreams = jnp.stack([buffers[0][1], buffers[1][1]])
    val_grads = jnp.stack([buffers[0][2], buffers[1][2]])
    flat_in = inputs.reshape(2, micro_count * length, model_width)
    flat_up = upstreams.reshape(2, micro_count * length, model_width)
    flat_mix = mixtures.reshape(2, micro_count * length, head_size)
    flat_vg = val_grads.reshape(2, micro_count * length, head_size)
    grad_value = jnp.einsum("ntd,nth->dnh", flat_in, flat_vg, preferred_element_type=jnp.float32)
    grad_output = jnp.einsum("ntd,nth->dnh", flat_up, flat_mix, preferred_element_type=jnp.float32)
    summed = lax.psum_scatter(
        jnp.stack([grad_value, grad_output], axis=2).reshape(
            model_width // lax.axis_size("dp") * lax.axis_size("dp"), 4 * head_size
        ),
        "dp",
        scatter_dimension=0,
        tiled=True,
    )
    summed = summed.reshape(-1, 2, 2, head_size)
    own_part = summed[:, 0]
    mirror_part = summed[:, 1]
    for bit_no in range(sections.bit_length() - 1):
        mirror_part = from_partner(mirror_part.astype(jnp.bfloat16), "section", bit_no).astype(
            mirror_part.dtype
        )
    combined = own_part + mirror_part
    weight_grads = jnp.transpose(combined, (1, 0, 2))[None]
    return (grads_in[None], weight_grads)


def swapped(block, axis, mask):
    return lax.ppermute(block, axis, [(i, i ^ mask) for i in range(lax.axis_size(axis))])


def shifted(block, distance):
    count = lax.axis_size("dp")
    return lax.ppermute(block, "dp", [(i, (i + 2 * distance) % count) for i in range(count)])


def contract(left, right, left_dim, right_dim):
    return lax.dot_general(
        left, right, (((left_dim,), (right_dim,)), ((), ())), preferred_element_type=jnp.float32
    )


def heads_kernel(length, valid, inputs, cot, held, queries, key_vectors, out, sums):
    tokens, head = queries.shape[1:]
    for way in range(2):
        for which, source in enumerate((inputs, cot)):
            term = contract(source[way], held[way, which], 1, 0)
            first = pl.program_id(0) == 0

            @pl.when(first)
            def _():
                sums[which, way] = term

            @pl.when(jnp.logical_not(first))
            def _():
                sums[which, way] += term

    @pl.when(pl.program_id(0) == pl.num_programs(0) - 1)
    def _():
        row = lax.broadcasted_iota(jnp.int32, (tokens, tokens), 0)
        col = lax.broadcasted_iota(jnp.int32, (tokens, tokens), 1)
        out[2 * tokens : 3 * tokens, :] = jnp.zeros((tokens, head), jnp.bfloat16)
        for way in range(2):
            scores = contract(queries[way], key_vectors[way], 1, 1) / math.sqrt(head)
            allowed = None
            for seq in range(tokens // length):
                start = seq * length
                here = (row >= start) & (row < start + length) & (col >= start) & (col <= row)
                here &= col - start < valid[way, seq]
                allowed = here if allowed is None else allowed | here
            scores = jnp.where(allowed, scores, -jnp.inf)
            row_max = jnp.max(scores, axis=-1, keepdims=True)
            raised = jnp.where(allowed, jnp.exp(scores - row_max), 0.0)
            attend = (raised / jnp.sum(raised, axis=-1, keepdims=True)).astype(jnp.bfloat16)
            mixture = contract(attend, sums[0, way].astype(jnp.bfloat16), 1, 0)
            out[way * tokens : (way + 1) * tokens, :] = sums[1, way].astype(jnp.bfloat16)
            out[2 * tokens : 3 * tokens, way * tokens : (way + 1) * tokens] = attend
            rows = slice((3 + way) * tokens, (4 + way) * tokens)
            out[rows, :] = mixture.astype(jnp.bfloat16)


def pack_kernel(near, far, tail, short, full):
    head = near.shape[-1]
    rows = near.shape[0] * head
    total = (near[...] + far[...]).astype(jnp.bfloat16).reshape(rows, head)
    short[:rows, :] = total
    full[:rows, :] = total
    short[rows:, :] = tail[: short.shape[0] - rows, :]
    full[rows:, :] = tail[...]


def chain_kernel(sections, tokens, head, place, *refs):
    parts = refs[:sections]
    gathered, steer, own = refs[sections:]
    products = (sections - 1) * head

    def at(here):
        mine = [[None] * sections, [None] * sections]
        for way in range(2):
            order = range(sections - 1, -1, -1) if way == 0 else range(sections)
            done = []
            for holder in order:
                part = parts[here ^ holder]
                first = products + way * tokens
                total = part[first : first + tokens, :].astype(jnp.float32)
                for other in done:
                    block = (other ^ holder) - 1
                    total += contract(
                        mine[way][other], part[block * head : (block + 1) * head, :], 1, 0
                    )
                base = products + 2 * tokens
                weights = part[base : base + tokens, way * tokens : (way + 1) * tokens]
                mine[way][holder] = contract(weights, total.astype(jnp.bfloat16), 0, 0).astype(
                    jnp.bfloat16
                )
                done.append(holder)
        zero = jnp.zeros((tokens, head), jnp.bfloat16)
        for far in range(sections):
            inside = here + far < sections
            gathered[0, far] = mine[0][here + far] if inside else zero
            gathered[1, far] = mine[1][sections - 1 - here - far] if inside else zero
        mirror = here ^ (sections - 1)
        base = products + 2 * tokens + tokens
        gathered[0, sections] = parts[0][base : base + tokens, :]
        gathered[1, sections] = parts[here ^ mirror][base + tokens : base + 2 * tokens, :]
        for way in range(2):
            own[way] = mine[way][here]
        for mask in range(1, sections):
            other = here ^ mask
            way = 0 if other > here else 1
            lanes = slice((mask - 1) * head, mask * head)
            steer[way * tokens : (way + 1) * tokens, lanes] = mine[way][other]
            steer[(1 - way) * tokens : (2 - way) * tokens, lanes] = zero

    for here in range(sections):

        @pl.when(place[0] == here)
        def _():
            at(here)


def input_kernel(sections, tokens, place, cot, steer, own, held, *refs):
    near, far = refs[: sections - 1], refs[sections - 1 : 2 * sections - 2]
    out = refs[2 * sections - 2]
    width = near[0].shape[1]
    core = place[1]
    for which, fetched in ((core, near), (1 - core, far)):
        start = pl.multiple_of(which * width, 128)
        weights = jnp.concatenate([block[0] for block in fetched], axis=1)
        total = contract(steer[...], weights, 1, 1)
        for way in range(2):
            branch = contract(own[way], held[way, pl.ds(start, width), :], 1, 1)
            branch += total[way * tokens : (way + 1) * tokens]
            base = cot[way, :, pl.ds(start, width)].astype(jnp.float32)
            out[way, :, pl.ds(start, width)] = (base + branch).astype(jnp.bfloat16)


def pick_weights(sections, place, halved, *refs):
    outs, sems = refs[: sections - 1], refs[sections - 1]
    here, core = place[0], place[1]
    copies = []
    for mask in range(sections - 1, 0, -1):
        way = jnp.where((here ^ mask) < here, 0, 1)
        copy = pltpu.make_async_copy(
            halved.at[way, 0, :, core], outs[mask - 1], sems.at[mask - 1]
        )
        copy.start()
        copies.append(copy)
    for copy in copies:
        copy.wait()


def carried_out(copies):
    for copy in copies:
        copy.start()
    for copy in copies:
        copy.wait()


def pick_outputs(place, halved, whole, out, own, part, sems):
    carried_out(
        [
            pltpu.make_async_copy(halved.at[1, 0, place[2], place[1]], part, sems.at[2]),
            pltpu.make_async_copy(halved.at[:, 1, :, place[1]], out, sems.at[0]),
            pltpu.make_async_copy(whole.at[:, 0], own, sems.at[1]),
        ]
    )


def pick_columns(steps, width, place, inputs, cot, *refs):
    outs, sems = refs[:steps], refs[steps]
    copies = []
    for distance in range(steps):
        start = pl.multiple_of((place[2] + distance) % steps * 2 * width, 128)
        copies.append(
            pltpu.make_async_copy(
                inputs.at[:, :, pl.ds(start, 2 * width)],
                outs[distance].at[0:2],
                sems.at[3 * distance],
            )
        )
        for way in range(2):
            half = pl.multiple_of(start + place[3 + way] * width, 128)
            copies.append(
                pltpu.make_async_copy(
                    cot.at[way, :, pl.ds(half, width)],
                    outs[distance].at[2, :, way * width : (way + 1) * width],
                    sems.at[3 * distance + 1 + way],
                )
            )
    carried_out(copies)


def pick_moving(steps, *refs):
    sources, upward, sems = refs[:steps], refs[steps], refs[steps + 3]
    width = upward.shape[-1] // 2
    copies = []
    for step, source in enumerate(sources):
        copies.append(pltpu.make_async_copy(source.at[1], upward.at[step], sems.at[3 * step]))
        for way in range(2):
            half = source.at[2, :, way * width : (way + 1) * width]
            copies.append(
                pltpu.make_async_copy(
                    half, refs[steps + 1 + way].at[step], sems.at[3 * step + 1 + way]
                )
            )
    carried_out(copies)


def product_kernel(sections, steps, place, outputs, *refs):
    fetched, out = refs[: sections - 1], refs[sections - 1]
    for mask in range(1, sections):
        way = jnp.where((place[0] ^ mask) > place[0], 0, 1)
        total = None
        for step in range(steps):
            term = contract(fetched[mask - 1][step], outputs[way, step], 0, 0)
            total = term if total is None else total + term
        out[mask - 1] = total


def weight_kernel(sections, steps, tokens, place, *refs):
    columns = refs[: 2 * steps]
    mirrored, lent = refs[2 * steps : 2 * steps + 2], refs[2 * steps + 2 : 2 * steps + 6]
    sent = refs[2 * steps + 6 : 4 * steps + 6]
    refs = refs[4 * steps + 6 :]
    own_slice, fetched, lent_slices = refs[0], refs[:sections], refs[sections - 1 :]
    out, lefts, rights, steers = refs[2 * sections - 1 :]
    width, head = out.shape[1:]
    every = 2 * steps * tokens
    lanes = pl.ds(pl.multiple_of(place[1] * width, 128), width)
    for index in range(2 * steps):
        rows = slice(index * tokens, (index + 1) * tokens)
        for way in range(2):
            for far in range(1, sections):
                steers[way, rows, (far - 1) * head : far * head] = sent[index][way, far]
            both = slice(way * every + index * tokens, way * every + (index + 1) * tokens)
            lefts[0, both, :] = sent[index][way, 0]
            lefts[1, both, :] = sent[index][way, sections]
        rights[rows, :] = columns[index][0, :, lanes]
        rows = slice(every + index * tokens, every + (index + 1) * tokens)
        rights[rows, :] = mirrored[index // steps][index % steps, :, lanes]
    out[0] = contract(lefts[0], rights[...], 0, 0).T
    for index in range(2 * steps):
        for way in range(2):
            both = slice(way * every + index * tokens, way * every + (index + 1) * tokens)
            half = slice(way * width, (way + 1) * width)

            @pl.when(place[3 + way] == place[1])
            def _():
                rights[both, :] = columns[index][2, :, half]

            @pl.when(place[3 + way] != place[1])
            def _():
                rights[both, :] = lent[2 * (index // steps) + way][index % steps]

    def corrected(here, way):
        rows = slice(way * every, (way + 1) * every)
        total = rights[rows, :].astype(jnp.float32)
        for far in range(1, sections - here):
            holder = here + far if way == 0 else sections - 1 - here - far
            if holder == here:
                held = own_slice[...]
            elif way == 1 and holder > here:
                held = lent_slices[holder ^ here][...]
            else:
                held = fetched[holder ^ here][place[2]]
            steer = steers[way, :, (far - 1) * head : far * head]
            total += contract(steer, held, 1, 1)
        rights[rows, :] = total.astype(jnp.bfloat16)

    for here in range(sections - 1):

        @pl.when(place[0] == here)
        def _():
            for way in range(2):
                corrected(here, way)

    out[1] = contract(lefts[1], rights[...], 0, 0).T


def gathered(layer_inputs, saved_queries, saved_keys, held_weights, cotangent, valid_lengths):
    sections = lax.axis_size("section")
    replicas = lax.axis_size("dp")
    steps = replicas // 2
    here = lax.axis_index("section")
    core = lax.axis_index("dp") % 2
    depth = lax.axis_index("dp") // 2
    inputs = layer_inputs[0]
    held = held_weights[0]
    seqs, length, model_width = inputs.shape[1:]
    tokens = seqs * length
    head = held.shape[-1]
    width = model_width // replicas
    inputs = inputs.reshape(2, tokens, model_width)
    cot = cotangent.reshape(2, tokens, model_width)
    halved = held.reshape(2, 2, steps, 2, width, head)
    asides = (sections // 2, 1)
    place = jnp.stack([here, core, depth] + [jnp.where(here & aside, 1, 0) for aside in asides])
    memory = pl.BlockSpec(memory_space=pltpu.VMEM)
    scalars = pl.BlockSpec(memory_space=pltpu.SMEM)
    anywhere = pl.BlockSpec(memory_space=pl.ANY)
    hbm = pl.BlockSpec(memory_space=pltpu.HBM)

    picked = pl.pallas_call(
        functools.partial(pick_weights, sections),
        in_specs=[scalars, hbm],
        out_specs=[memory] * (sections - 1),
        out_shape=[jax.ShapeDtypeStruct((steps, width, head), jnp.bfloat16)] * (sections - 1),
        scratch_shapes=[pltpu.SemaphoreType.DMA((sections - 1,))],
        name="pick_weights",
        compiler_params=pltpu.CompilerParams(vmem_limit_bytes=52 << 20),
    )(place, halved)
    fetched = [None] * sections
    for mask in range(sections - 1, 0, -1):
        fetched[mask] = swapped(picked[mask - 1], "section", mask)

    picked = pl.pallas_call(
        functools.partial(pick_columns, steps, width),
        in_specs=[scalars] + [hbm] * 2,
        out_specs=[memory] * steps,
        out_shape=[jax.ShapeDtypeStruct((3, tokens, 2 * width), jnp.bfloat16)] * steps,
        scratch_shapes=[pltpu.SemaphoreType.DMA((3 * steps,))],
        name="pick_columns",
        compiler_params=pltpu.CompilerParams(vmem_limit_bytes=52 << 20),
    )(place, inputs, cot)
    near_columns = [picked[0]]
    for distance in range(1, steps):
        near_columns.append(shifted(picked[distance], distance))

    lengths = valid_lengths
    blocks = 4
    cut = model_width // blocks
    tail = pl.pallas_call(
        functools.partial(heads_kernel, length),
        grid=(blocks,),
        in_specs=[
            scalars,
            pl.BlockSpec((2, tokens, cut), lambda i: (0, 0, i)),
            pl.BlockSpec((2, tokens, cut), lambda i: (0, 0, i)),
            pl.BlockSpec((2, 2, cut, head), lambda i: (0, 0, i, 0)),
            pl.BlockSpec((2, tokens, head), lambda i: (0, 0, 0)),
            pl.BlockSpec((2, tokens, head), lambda i: (0, 0, 0)),
        ],
        out_specs=pl.BlockSpec((5 * tokens, head), lambda i: (0, 0)),
        out_shape=jax.ShapeDtypeStruct((5 * tokens, head), jnp.bfloat16),
        scratch_shapes=[pltpu.VMEM((2, 2, tokens, head), jnp.float32)],
        name="heads",
        compiler_params=pltpu.CompilerParams(vmem_limit_bytes=12 << 20),
    )(
        lengths,
        inputs,
        cot,
        held,
        saved_queries[0].reshape(2, tokens, head),
        saved_keys[0].reshape(2, tokens, head),
    )

    outputs, own_values, own_slice = pl.pallas_call(
        pick_outputs,
        in_specs=[scalars, hbm, hbm],
        out_specs=[memory] * 3,
        out_shape=[
            jax.ShapeDtypeStruct((2, steps, width, head), jnp.bfloat16),
            jax.ShapeDtypeStruct((2, model_width, head), jnp.bfloat16),
            jax.ShapeDtypeStruct((width, head), jnp.bfloat16),
        ],
        scratch_shapes=[pltpu.SemaphoreType.DMA((3,))],
        name="pick_outputs",
        compiler_params=pltpu.CompilerParams(vmem_limit_bytes=8 << 20),
    )(place, halved, held)
    products = pl.pallas_call(
        functools.partial(product_kernel, sections, steps),
        in_specs=[scalars] + [memory] * sections,
        out_specs=memory,
        out_shape=jax.ShapeDtypeStruct((sections - 1, head, head), jnp.float32),
        name="products",
        compiler_params=pltpu.CompilerParams(vmem_limit_bytes=8 << 20),
    )(place, outputs, *fetched[1:])
    far_products = swapped(products, "dp", 1)
    lent_back = [None] * sections
    for mask in range(1, sections):
        lent_back[mask] = swapped(fetched[mask], "dp", 1)

    rows = (sections - 1) * head + 3 * tokens
    short, full = pl.pallas_call(
        pack_kernel,
        in_specs=[memory] * 3,
        out_specs=[memory] * 2,
        out_shape=[
            jax.ShapeDtypeStruct((rows, head), jnp.bfloat16),
            jax.ShapeDtypeStruct((rows + 2 * tokens, head), jnp.bfloat16),
        ],
        name="pack",
        compiler_params=pltpu.CompilerParams(vmem_limit_bytes=8 << 20),
    )(products, far_products, tail)
    parts = [full]
    for mask in range(1, sections):
        parts.append(swapped(full if mask == sections - 1 else short, "section", mask))

    upward, *sideways = pl.pallas_call(
        functools.partial(pick_moving, steps),
        in_specs=[anywhere] * steps,
        out_specs=[memory] * 3,
        out_shape=[jax.ShapeDtypeStruct((steps, tokens, 2 * width), jnp.bfloat16)]
        + [jax.ShapeDtypeStruct((steps, tokens, width), jnp.bfloat16)] * 2,
        scratch_shapes=[pltpu.SemaphoreType.DMA((3 * steps,))],
        name="pick_moving",
        compiler_params=pltpu.CompilerParams(vmem_limit_bytes=8 << 20),
    )(*near_columns)
    near_mirror = swapped(upward, "section", sections - 1)
    near_aside, far_aside = [], []
    for way in range(2):
        near_aside.append(swapped(sideways[way], "section", asides[way]))
    far_mirror = swapped(near_mirror, "dp", 1)
    for way in range(2):
        far_aside.append(swapped(near_aside[way], "dp", 1))
    far_columns = []
    for distance in range(steps):
        far_columns.append(swapped(near_columns[distance], "dp", 1))
    lent = [own_slice]
    for mask in range(1, sections):
        route = [
            (i, i ^ mask) for i in range(sections) if i ^ mask < i < sections - 1 - (i ^ mask)
        ]
        lent.append(lax.ppermute(own_slice, "section", route) if route else own_slice)

    sent, steer, own = pl.pallas_call(
        functools.partial(chain_kernel, sections, tokens, head),
        in_specs=[scalars] + [memory] * sections,
        out_specs=(memory, memory, memory),
        out_shape=(
            jax.ShapeDtypeStruct((2, sections + 1, tokens, head), jnp.bfloat16),
            jax.ShapeDtypeStruct((2 * tokens, (sections - 1) * head), jnp.bfloat16),
            jax.ShapeDtypeStruct((2, tokens, head), jnp.bfloat16),
        ),
        name="chain",
        compiler_params=pltpu.CompilerParams(vmem_limit_bytes=8 << 20),
    )(place, *parts)

    near_sent = [sent]
    for distance in range(1, steps):
        near_sent.append(shifted(sent, distance))
    far_sent = []
    for distance in range(steps):
        far_sent.append(swapped(near_sent[distance], "dp", 1))

    grads_in = pl.pallas_call(
        functools.partial(input_kernel, sections, tokens),
        grid=(steps,),
        in_specs=[
            scalars,
            pl.BlockSpec((2, tokens, 2 * width), lambda i: (0, 0, i)),
            pl.BlockSpec((2 * tokens, (sections - 1) * head), lambda i: (0, 0)),
            pl.BlockSpec((2, tokens, head), lambda i: (0, 0, 0)),
            pl.BlockSpec((2, 2 * width, head), lambda i: (0, i, 0)),
        ]
        + [pl.BlockSpec((1, width, head), lambda i: (i, 0, 0))] * (2 * sections - 2),
        out_specs=pl.BlockSpec((2, tokens, 2 * width), lambda i: (0, 0, i)),
        out_shape=jax.ShapeDtypeStruct((2, tokens, model_width), jnp.bfloat16),
        name="input_side",
        compiler_params=pltpu.CompilerParams(vmem_limit_bytes=12 << 20),
    )(place, cot, steer, own, own_values, *fetched[1:], *lent_back[1:])

    every = replicas * tokens
    weight_grads = pl.pallas_call(
        functools.partial(weight_kernel, sections, steps, tokens),
        in_specs=[scalars] + [memory] * (4 * steps + 2 * sections + 5),
        out_specs=memory,
        out_shape=jax.ShapeDtypeStruct((2, width, head), jnp.float32),
        scratch_shapes=[
            pltpu.VMEM((2, 2 * every, head), jnp.bfloat16),
            pltpu.VMEM((2 * every, width), jnp.bfloat16),
            pltpu.VMEM((2, every, (sections - 1) * head), jnp.bfloat16),
        ],
        name="weight_side",
        compiler_params=pltpu.CompilerParams(vmem_limit_bytes=20 << 20),
    )(
        place,
        *near_columns,
        *far_columns,
        near_mirror,
        far_mirror,
        *near_aside,
        *far_aside,
        *near_sent,
        *far_sent,
        own_slice,
        *fetched[1:],
        *lent[1:],
    )
    shape = (1, 2, seqs, length, model_width)
    return (grads_in.reshape(shape), weight_grads[None])


def shards(*operands):
    layer_inputs, held_weights = operands[0], operands[3]
    sections = lax.axis_size("section")
    replicas = lax.axis_size("dp")
    seqs, length, model_width = layer_inputs.shape[2:]
    head = held_weights.shape[-1]
    every_token = replicas * seqs * length
    moved = 2 * every_token * ((sections + 1) * head + 2 * model_width // replicas) * 2
    partial_sums = 4 * model_width * head * 4
    even = replicas % 2 == 0 and sections > 1 and sections & (sections - 1) == 0
    if even and moved < partial_sums and 2 * seqs * length <= head:
        return gathered(*operands)
    return reduced(*operands)


def solution(mesh):
    return jax.shard_map(
        shards,
        mesh=mesh,
        in_specs=(
            P("section", None, "dp", None, None),
            P("section", None, "dp", None, None),
            P("section", None, "dp", None, None),
            P("section", None, None, None, None),
            P(None, "dp", None, None),
            P(None, "dp"),
        ),
        out_specs=(P("section", None, "dp", None, None), P("section", None, "dp", None)),
        check_vma=False,
    )
```

```python
import functools
import math

import jax
import jax.numpy as jnp
from jax import lax
from jax.experimental import pallas as pl
from jax.experimental.pallas import tpu as pltpu
from jax.sharding import PartitionSpec as P


def passed_along(block, axis, distance):
    devices = range(lax.axis_size(axis))
    route = [(i - distance, i) for i in devices if i - distance in devices]
    return lax.ppermute(block, axis, route)


def from_partner(block, axis, bit):
    count = lax.axis_size(axis)
    route = []
    for low in range(count):
        high = low | 1 << bit
        if high != low and high < count:
            route += [(low, high), (high, low)]
    return lax.ppermute(block, axis, route)


def attention_weights(queries, key_vectors, valid_lengths):
    length = queries.shape[-2]
    scores = jnp.einsum(
        "nmth,nmsh->nmts", queries, key_vectors, preferred_element_type=jnp.float32
    ) / math.sqrt(queries.shape[-1])
    row_pos = lax.broadcasted_iota(jnp.int32, (length, length), 0)
    col_pos = lax.broadcasted_iota(jnp.int32, (length, length), 1)
    allowed = (col_pos <= row_pos)[None, None] & (
        col_pos[None, None] < valid_lengths[:, :, None, None]
    )
    scores = jnp.where(allowed, scores, -jnp.inf)
    row_max = jnp.max(scores, axis=-1, keepdims=True)
    raised = jnp.where(allowed, jnp.exp(scores - row_max), 0.0)
    return (raised / jnp.sum(raised, axis=-1, keepdims=True)).astype(jnp.bfloat16)


def reduced(layer_inputs, saved_queries, saved_keys, held_weights, cotangent, valid_lengths):
    sections = lax.axis_size("section")
    position = lax.axis_index("section")
    inputs = layer_inputs[0]
    value_w = held_weights[0, :, 0]
    output_w = held_weights[0, :, 1]
    attend = attention_weights(saved_queries[0], saved_keys[0], valid_lengths)
    micro_count = inputs.shape[1]
    length = inputs.shape[2]
    model_width = inputs.shape[3]
    head_size = value_w.shape[2]
    values = jnp.einsum(
        "nmld,ndh->nmlh", inputs, value_w, preferred_element_type=jnp.float32
    ).astype(jnp.bfloat16)
    mixtures = jnp.einsum(
        "nmts,nmsh->nmth", attend, values, preferred_element_type=jnp.float32
    ).astype(jnp.bfloat16)
    is_end = [position == sections - 1, position == 0]
    starts = [sections - 1 - position, position]

    def make_compute(direction):

        def compute(operands):
            grads, uppers, vgrads, incoming, index = operands
            fresh = lax.dynamic_index_in_dim(cotangent[direction], index, 0, keepdims=False)
            upstream = jnp.where(is_end[direction], fresh, incoming)
            weights_now = lax.dynamic_index_in_dim(attend[direction], index, 0, keepdims=False)
            out_grad = jnp.dot(
                upstream, output_w[direction], preferred_element_type=jnp.float32
            ).astype(jnp.bfloat16)
            val_grad = jnp.einsum(
                "ts,th->sh", weights_now, out_grad, preferred_element_type=jnp.float32
            ).astype(jnp.bfloat16)
            branch = jnp.einsum(
                "lh,dh->ld", val_grad, value_w[direction], preferred_element_type=jnp.float32
            )
            grad_input = (upstream.astype(jnp.float32) + branch).astype(jnp.bfloat16)
            grads = lax.dynamic_update_index_in_dim(grads, grad_input, index, 0)
            uppers = lax.dynamic_update_index_in_dim(uppers, upstream, index, 0)
            vgrads = lax.dynamic_update_index_in_dim(vgrads, val_grad, index, 0)
            return (grad_input, (grads, uppers, vgrads))

        return compute

    def skip(operands):
        grads, uppers, vgrads, incoming, _ = operands
        return (jnp.zeros_like(incoming), (grads, uppers, vgrads))

    def advance(moment, received, buffers):
        outgoing = []
        updated = []
        for direction in range(2):
            micro_id = moment - starts[direction]
            active = (micro_id >= 0) & (micro_id < micro_count)
            clipped = jnp.clip(micro_id, 0, micro_count - 1)
            grads, uppers, vgrads = buffers[direction]
            sent_now, fresh_buffers = lax.cond(
                active,
                make_compute(direction),
                skip,
                (grads, uppers, vgrads, received[direction], clipped),
            )
            outgoing.append(sent_now)
            updated.append(fresh_buffers)
        return (jnp.stack(outgoing), tuple(updated))

    big_zero = jnp.zeros((micro_count, length, model_width), jnp.bfloat16)
    small_zero = jnp.zeros((micro_count, length, head_size), jnp.bfloat16)
    buffers = ((big_zero, big_zero, small_zero), (big_zero, big_zero, small_zero))
    sent, buffers = advance(
        jnp.int32(0), jnp.zeros((2, length, model_width), jnp.bfloat16), buffers
    )

    def loop_body(moment, carried):
        outgoing, held = carried
        from_next = passed_along(outgoing[0], "section", -1)
        from_prev = passed_along(outgoing[1], "section", 1)
        return advance(moment, jnp.stack([from_next, from_prev]), held)

    sent, buffers = lax.fori_loop(1, sections + micro_count - 1, loop_body, (sent, buffers))
    grads_in = jnp.stack([buffers[0][0], buffers[1][0]])
    upstreams = jnp.stack([buffers[0][1], buffers[1][1]])
    val_grads = jnp.stack([buffers[0][2], buffers[1][2]])
    flat_in = inputs.reshape(2, micro_count * length, model_width)
    flat_up = upstreams.reshape(2, micro_count * length, model_width)
    flat_mix = mixtures.reshape(2, micro_count * length, head_size)
    flat_vg = val_grads.reshape(2, micro_count * length, head_size)
    grad_value = jnp.einsum("ntd,nth->dnh", flat_in, flat_vg, preferred_element_type=jnp.float32)
    grad_output = jnp.einsum("ntd,nth->dnh", flat_up, flat_mix, preferred_element_type=jnp.float32)
    summed = lax.psum_scatter(
        jnp.stack([grad_value, grad_output], axis=2).reshape(
            model_width // lax.axis_size("dp") * lax.axis_size("dp"), 4 * head_size
        ),
        "dp",
        scatter_dimension=0,
        tiled=True,
    )
    summed = summed.reshape(-1, 2, 2, head_size)
    own_part = summed[:, 0]
    mirror_part = summed[:, 1]
    for bit_no in range(sections.bit_length() - 1):
        mirror_part = from_partner(mirror_part.astype(jnp.bfloat16), "section", bit_no).astype(
            mirror_part.dtype
        )
    combined = own_part + mirror_part
    weight_grads = jnp.transpose(combined, (1, 0, 2))[None]
    return (grads_in[None], weight_grads)


def swapped(block, axis, mask):
    return lax.ppermute(block, axis, [(i, i ^ mask) for i in range(lax.axis_size(axis))])


def shifted(block, distance):
    count = lax.axis_size("dp")
    return lax.ppermute(block, "dp", [(i, (i + 2 * distance) % count) for i in range(count)])


def contract(left, right, left_dim, right_dim):
    return lax.dot_general(
        left, right, (((left_dim,), (right_dim,)), ((), ())), preferred_element_type=jnp.float32
    )


def heads_kernel(length, valid, inputs, cot, held, queries, key_vectors, out, sums):
    tokens, head = queries.shape[1:]
    for way in range(2):
        for which, source in enumerate((inputs, cot)):
            term = contract(source[way], held[way, which], 1, 0)
            first = pl.program_id(0) == 0

            @pl.when(first)
            def _():
                sums[which, way] = term

            @pl.when(jnp.logical_not(first))
            def _():
                sums[which, way] += term

    @pl.when(pl.program_id(0) == pl.num_programs(0) - 1)
    def _():
        row = lax.broadcasted_iota(jnp.int32, (tokens, tokens), 0)
        col = lax.broadcasted_iota(jnp.int32, (tokens, tokens), 1)
        out[2 * tokens : 3 * tokens, :] = jnp.zeros((tokens, head), jnp.bfloat16)
        for way in range(2):
            scores = contract(queries[way], key_vectors[way], 1, 1) / math.sqrt(head)
            allowed = None
            for seq in range(tokens // length):
                start = seq * length
                here = (row >= start) & (row < start + length) & (col >= start) & (col <= row)
                here &= col - start < valid[way, seq]
                allowed = here if allowed is None else allowed | here
            scores = jnp.where(allowed, scores, -jnp.inf)
            row_max = jnp.max(scores, axis=-1, keepdims=True)
            raised = jnp.where(allowed, jnp.exp(scores - row_max), 0.0)
            attend = (raised / jnp.sum(raised, axis=-1, keepdims=True)).astype(jnp.bfloat16)
            mixture = contract(attend, sums[0, way].astype(jnp.bfloat16), 1, 0)
            out[way * tokens : (way + 1) * tokens, :] = sums[1, way].astype(jnp.bfloat16)
            out[2 * tokens : 3 * tokens, way * tokens : (way + 1) * tokens] = attend
            rows = slice((3 + way) * tokens, (4 + way) * tokens)
            out[rows, :] = mixture.astype(jnp.bfloat16)


def pack_kernel(near, far, tail, short, full):
    head = near.shape[-1]
    rows = near.shape[0] * head
    total = (near[...] + far[...]).astype(jnp.bfloat16).reshape(rows, head)
    short[:rows, :] = total
    full[:rows, :] = total
    short[rows:, :] = tail[: short.shape[0] - rows, :]
    full[rows:, :] = tail[...]


def chain_kernel(sections, tokens, head, place, *refs):
    parts = refs[:sections]
    gathered, steer, own = refs[sections:]
    products = (sections - 1) * head

    def at(here):
        mine = [[None] * sections, [None] * sections]
        for way in range(2):
            order = range(sections - 1, -1, -1) if way == 0 else range(sections)
            done = []
            for holder in order:
                part = parts[here ^ holder]
                first = products + way * tokens
                total = part[first : first + tokens, :].astype(jnp.float32)
                for other in done:
                    block = (other ^ holder) - 1
                    total += contract(
                        mine[way][other], part[block * head : (block + 1) * head, :], 1, 0
                    )
                base = products + 2 * tokens
                weights = part[base : base + tokens, way * tokens : (way + 1) * tokens]
                mine[way][holder] = contract(weights, total.astype(jnp.bfloat16), 0, 0).astype(
                    jnp.bfloat16
                )
                done.append(holder)
        zero = jnp.zeros((tokens, head), jnp.bfloat16)
        for far in range(sections):
            inside = here + far < sections
            gathered[0, far] = mine[0][here + far] if inside else zero
            gathered[1, far] = mine[1][sections - 1 - here - far] if inside else zero
        mirror = here ^ (sections - 1)
        base = products + 2 * tokens + tokens
        gathered[0, sections] = parts[0][base : base + tokens, :]
        gathered[1, sections] = parts[here ^ mirror][base + tokens : base + 2 * tokens, :]
        for way in range(2):
            own[way] = mine[way][here]
        for mask in range(1, sections):
            other = here ^ mask
            way = 0 if other > here else 1
            lanes = slice((mask - 1) * head, mask * head)
            steer[way * tokens : (way + 1) * tokens, lanes] = mine[way][other]
            steer[(1 - way) * tokens : (2 - way) * tokens, lanes] = zero

    for here in range(sections):

        @pl.when(place[0] == here)
        def _():
            at(here)


def input_kernel(sections, tokens, place, cot, steer, own, held, *refs):
    near, far = refs[: sections - 1], refs[sections - 1 : 2 * sections - 2]
    out = refs[2 * sections - 2]
    width = near[0].shape[1]
    core = place[1]
    for which, fetched in ((core, near), (1 - core, far)):
        start = pl.multiple_of(which * width, 128)
        weights = jnp.concatenate([block[0] for block in fetched], axis=1)
        total = contract(steer[...], weights, 1, 1)
        for way in range(2):
            branch = contract(own[way], held[way, pl.ds(start, width), :], 1, 1)
            branch += total[way * tokens : (way + 1) * tokens]
            base = cot[way, :, pl.ds(start, width)].astype(jnp.float32)
            out[way, :, pl.ds(start, width)] = (base + branch).astype(jnp.bfloat16)


def pick_weights(sections, place, halved, *refs):
    outs, sems = refs[: sections - 1], refs[sections - 1]
    here, core = place[0], place[1]
    copies = []
    for mask in range(sections - 1, 0, -1):
        way = jnp.where((here ^ mask) < here, 0, 1)
        copy = pltpu.make_async_copy(
            halved.at[way, 0, :, core], outs[mask - 1], sems.at[mask - 1]
        )
        copy.start()
        copies.append(copy)
    for copy in copies:
        copy.wait()


def carried_out(copies):
    for copy in copies:
        copy.start()
    for copy in copies:
        copy.wait()


def pick_outputs(place, halved, whole, out, own, part, sems):
    carried_out(
        [
            pltpu.make_async_copy(halved.at[1, 0, place[2], place[1]], part, sems.at[2]),
            pltpu.make_async_copy(halved.at[:, 1, :, place[1]], out, sems.at[0]),
            pltpu.make_async_copy(whole.at[:, 0], own, sems.at[1]),
        ]
    )


def pick_columns(steps, width, place, inputs, cot, *refs):
    outs, halves, sems = refs[:steps], refs[steps : 2 * steps], refs[2 * steps]
    copies = []
    for distance in range(steps):
        start = pl.multiple_of((place[2] + distance) % steps * 2 * width, 128)
        copies.append(
            pltpu.make_async_copy(
                inputs.at[:, :, pl.ds(start, 2 * width)], outs[distance], sems.at[3 * distance]
            )
        )
        for way in range(2):
            half = pl.multiple_of(start + place[3 + way] * width, 128)
            copies.append(
                pltpu.make_async_copy(
                    cot.at[way, :, pl.ds(half, width)],
                    halves[distance].at[way],
                    sems.at[3 * distance + 1 + way],
                )
            )
    carried_out(copies)


def pick_moving(steps, which, *refs):
    sources, outs, sems = refs[:steps], refs[steps:-1], refs[-1]
    copies = []
    for step, source in enumerate(sources):
        for index, out in zip(which, outs):
            copies.append(
                pltpu.make_async_copy(source.at[index], out.at[step], sems.at[len(copies)])
            )
    carried_out(copies)


def product_kernel(sections, steps, place, outputs, *refs):
    fetched, out = refs[: sections - 1], refs[sections - 1]
    for mask in range(1, sections):
        way = jnp.where((place[0] ^ mask) > place[0], 0, 1)
        total = None
        for step in range(steps):
            term = contract(fetched[mask - 1][step], outputs[way, step], 0, 0)
            total = term if total is None else total + term
        out[mask - 1] = total


def weight_kernel(sections, steps, tokens, place, *refs):
    columns = refs[: 2 * steps]
    halves, refs = refs[2 * steps : 4 * steps], refs[2 * steps :]
    mirrored, lent = refs[2 * steps : 2 * steps + 2], refs[2 * steps + 2 : 2 * steps + 6]
    sent = refs[2 * steps + 6 : 4 * steps + 6]
    refs = refs[4 * steps + 6 :]
    own_slice, fetched, lent_slices = refs[0], refs[:sections], refs[sections - 1 :]
    out, lefts, rights, steers = refs[2 * sections - 1 :]
    width, head = out.shape[1:]
    every = 2 * steps * tokens
    lanes = pl.ds(pl.multiple_of(place[1] * width, 128), width)
    for index in range(2 * steps):
        rows = slice(index * tokens, (index + 1) * tokens)
        for way in range(2):
            for far in range(1, sections):
                steers[way, rows, (far - 1) * head : far * head] = sent[index][way, far]
            both = slice(way * every + index * tokens, way * every + (index + 1) * tokens)
            lefts[0, both, :] = sent[index][way, 0]
            lefts[1, both, :] = sent[index][way, sections]
        rights[rows, :] = columns[index][0, :, lanes]
        rows = slice(every + index * tokens, every + (index + 1) * tokens)
        rights[rows, :] = mirrored[index // steps][index % steps, :, lanes]
    out[0] = contract(lefts[0], rights[...], 0, 0).T
    for index in range(2 * steps):
        for way in range(2):
            both = slice(way * every + index * tokens, way * every + (index + 1) * tokens)

            @pl.when(place[3 + way] == place[1])
            def _():
                rights[both, :] = halves[index][way]

            @pl.when(place[3 + way] != place[1])
            def _():
                rights[both, :] = lent[2 * (index // steps) + way][index % steps]

    def corrected(here, way):
        rows = slice(way * every, (way + 1) * every)
        blocks = []
        for far in range(1, sections - here):
            holder = here + far if way == 0 else sections - 1 - here - far
            if holder == here:
                blocks.append(own_slice[...])
            elif way == 1 and holder > here:
                blocks.append(lent_slices[holder ^ here][...])
            else:
                blocks.append(fetched[holder ^ here][place[2]])
        steer = steers[way, :, : len(blocks) * head]
        total = contract(steer, jnp.concatenate(blocks, axis=1), 1, 1)
        rights[rows, :] = (rights[rows, :].astype(jnp.float32) + total).astype(jnp.bfloat16)

    for here in range(sections - 1):

        @pl.when(place[0] == here)
        def _():
            for way in range(2):
                corrected(here, way)

    out[1] = contract(lefts[1], rights[...], 0, 0).T


def gathered(layer_inputs, saved_queries, saved_keys, held_weights, cotangent, valid_lengths):
    sections = lax.axis_size("section")
    replicas = lax.axis_size("dp")
    steps = replicas // 2
    here = lax.axis_index("section")
    core = lax.axis_index("dp") % 2
    depth = lax.axis_index("dp") // 2
    inputs = layer_inputs[0]
    held = held_weights[0]
    seqs, length, model_width = inputs.shape[1:]
    tokens = seqs * length
    head = held.shape[-1]
    width = model_width // replicas
    inputs = inputs.reshape(2, tokens, model_width)
    cot = cotangent.reshape(2, tokens, model_width)
    halved = held.reshape(2, 2, steps, 2, width, head)
    asides = (sections // 2, 1)
    place = jnp.stack([here, core, depth] + [jnp.where(here & aside, 1, 0) for aside in asides])
    memory = pl.BlockSpec(memory_space=pltpu.VMEM)
    scalars = pl.BlockSpec(memory_space=pltpu.SMEM)
    anywhere = pl.BlockSpec(memory_space=pl.ANY)
    hbm = pl.BlockSpec(memory_space=pltpu.HBM)

    picked = pl.pallas_call(
        functools.partial(pick_weights, sections),
        in_specs=[scalars, hbm],
        out_specs=[memory] * (sections - 1),
        out_shape=[jax.ShapeDtypeStruct((steps, width, head), jnp.bfloat16)] * (sections - 1),
        scratch_shapes=[pltpu.SemaphoreType.DMA((sections - 1,))],
        name="pick_weights",
        compiler_params=pltpu.CompilerParams(vmem_limit_bytes=52 << 20),
    )(place, halved)
    fetched = [None] * sections
    for mask in range(sections - 1, 0, -1):
        fetched[mask] = swapped(picked[mask - 1], "section", mask)

    wide = jax.ShapeDtypeStruct((2, tokens, 2 * width), jnp.bfloat16)
    slim = jax.ShapeDtypeStruct((2, tokens, width), jnp.bfloat16)
    picked = pl.pallas_call(
        functools.partial(pick_columns, steps, width),
        in_specs=[scalars] + [hbm] * 2,
        out_specs=[memory] * (2 * steps),
        out_shape=[wide] * steps + [slim] * steps,
        scratch_shapes=[pltpu.SemaphoreType.DMA((3 * steps,))],
        name="pick_columns",
        compiler_params=pltpu.CompilerParams(vmem_limit_bytes=52 << 20),
    )(place, inputs, cot)
    near_columns, near_halves = [picked[0]], [picked[steps]]
    for distance in range(1, steps):
        near_halves.append(shifted(picked[steps + distance], distance))
    for distance in range(1, steps):
        near_columns.append(shifted(picked[distance], distance))

    def moving(sources, which, shape):
        return pl.pallas_call(
            functools.partial(pick_moving, steps, which),
            in_specs=[anywhere] * steps,
            out_specs=[memory] * len(which),
            out_shape=[jax.ShapeDtypeStruct((steps,) + shape, jnp.bfloat16)] * len(which),
            scratch_shapes=[pltpu.SemaphoreType.DMA((steps * len(which),))],
            name="pick_moving",
            compiler_params=pltpu.CompilerParams(vmem_limit_bytes=8 << 20),
        )(*sources)

    sideways = moving(near_halves, (0, 1), (tokens, width))
    near_aside, far_aside, far_columns, far_halves = [], [], [], []
    for way in range(2):
        near_aside.append(swapped(sideways[way], "section", asides[way]))
    for way in range(2):
        far_aside.append(swapped(near_aside[way], "dp", 1))
    for distance in range(steps):
        far_halves.append(swapped(near_halves[distance], "dp", 1))

    lengths = valid_lengths
    blocks = 4
    cut = model_width // blocks
    tail = pl.pallas_call(
        functools.partial(heads_kernel, length),
        grid=(blocks,),
        in_specs=[
            scalars,
            pl.BlockSpec((2, tokens, cut), lambda i: (0, 0, i)),
            pl.BlockSpec((2, tokens, cut), lambda i: (0, 0, i)),
            pl.BlockSpec((2, 2, cut, head), lambda i: (0, 0, i, 0)),
            pl.BlockSpec((2, tokens, head), lambda i: (0, 0, 0)),
            pl.BlockSpec((2, tokens, head), lambda i: (0, 0, 0)),
        ],
        out_specs=pl.BlockSpec((5 * tokens, head), lambda i: (0, 0)),
        out_shape=jax.ShapeDtypeStruct((5 * tokens, head), jnp.bfloat16),
        scratch_shapes=[pltpu.VMEM((2, 2, tokens, head), jnp.float32)],
        name="heads",
        compiler_params=pltpu.CompilerParams(vmem_limit_bytes=12 << 20),
    )(
        lengths,
        inputs,
        cot,
        held,
        saved_queries[0].reshape(2, tokens, head),
        saved_keys[0].reshape(2, tokens, head),
    )

    outputs, own_values, own_slice = pl.pallas_call(
        pick_outputs,
        in_specs=[scalars, hbm, hbm],
        out_specs=[memory] * 3,
        out_shape=[
            jax.ShapeDtypeStruct((2, steps, width, head), jnp.bfloat16),
            jax.ShapeDtypeStruct((2, model_width, head), jnp.bfloat16),
            jax.ShapeDtypeStruct((width, head), jnp.bfloat16),
        ],
        scratch_shapes=[pltpu.SemaphoreType.DMA((3,))],
        name="pick_outputs",
        compiler_params=pltpu.CompilerParams(vmem_limit_bytes=8 << 20),
    )(place, halved, held)
    products = pl.pallas_call(
        functools.partial(product_kernel, sections, steps),
        in_specs=[scalars] + [memory] * sections,
        out_specs=memory,
        out_shape=jax.ShapeDtypeStruct((sections - 1, head, head), jnp.float32),
        name="products",
        compiler_params=pltpu.CompilerParams(vmem_limit_bytes=8 << 20),
    )(place, outputs, *fetched[1:])
    far_products = swapped(products, "dp", 1)
    lent_back = [None] * sections
    for mask in range(1, sections):
        lent_back[mask] = swapped(fetched[mask], "dp", 1)

    rows = (sections - 1) * head + 3 * tokens
    short, full = pl.pallas_call(
        pack_kernel,
        in_specs=[memory] * 3,
        out_specs=[memory] * 2,
        out_shape=[
            jax.ShapeDtypeStruct((rows, head), jnp.bfloat16),
            jax.ShapeDtypeStruct((rows + 2 * tokens, head), jnp.bfloat16),
        ],
        name="pack",
        compiler_params=pltpu.CompilerParams(vmem_limit_bytes=8 << 20),
    )(products, far_products, tail)
    parts = [full]
    for mask in range(1, sections):
        parts.append(swapped(full if mask == sections - 1 else short, "section", mask))

    (upward,) = moving(near_columns, (1,), (tokens, 2 * width))
    near_mirror = swapped(upward, "section", sections - 1)
    far_mirror = swapped(near_mirror, "dp", 1)
    for distance in range(steps):
        far_columns.append(swapped(near_columns[distance], "dp", 1))
    lent = [own_slice]
    for mask in range(1, sections):
        route = [
            (i, i ^ mask) for i in range(sections) if i ^ mask < i < sections - 1 - (i ^ mask)
        ]
        lent.append(lax.ppermute(own_slice, "section", route) if route else own_slice)

    sent, steer, own = pl.pallas_call(
        functools.partial(chain_kernel, sections, tokens, head),
        in_specs=[scalars] + [memory] * sections,
        out_specs=(memory, memory, memory),
        out_shape=(
            jax.ShapeDtypeStruct((2, sections + 1, tokens, head), jnp.bfloat16),
            jax.ShapeDtypeStruct((2 * tokens, (sections - 1) * head), jnp.bfloat16),
            jax.ShapeDtypeStruct((2, tokens, head), jnp.bfloat16),
        ),
        name="chain",
        compiler_params=pltpu.CompilerParams(vmem_limit_bytes=8 << 20),
    )(place, *parts)

    near_sent = [sent]
    for distance in range(1, steps):
        near_sent.append(shifted(sent, distance))
    far_sent = []
    for distance in range(steps):
        far_sent.append(swapped(near_sent[distance], "dp", 1))

    grads_in = pl.pallas_call(
        functools.partial(input_kernel, sections, tokens),
        grid=(steps,),
        in_specs=[
            scalars,
            pl.BlockSpec((2, tokens, 2 * width), lambda i: (0, 0, i)),
            pl.BlockSpec((2 * tokens, (sections - 1) * head), lambda i: (0, 0)),
            pl.BlockSpec((2, tokens, head), lambda i: (0, 0, 0)),
            pl.BlockSpec((2, 2 * width, head), lambda i: (0, i, 0)),
        ]
        + [pl.BlockSpec((1, width, head), lambda i: (i, 0, 0))] * (2 * sections - 2),
        out_specs=pl.BlockSpec((2, tokens, 2 * width), lambda i: (0, 0, i)),
        out_shape=jax.ShapeDtypeStruct((2, tokens, model_width), jnp.bfloat16),
        name="input_side",
        compiler_params=pltpu.CompilerParams(vmem_limit_bytes=12 << 20),
    )(place, cot, steer, own, own_values, *fetched[1:], *lent_back[1:])

    every = replicas * tokens
    weight_grads = pl.pallas_call(
        functools.partial(weight_kernel, sections, steps, tokens),
        in_specs=[scalars] + [memory] * (6 * steps + 2 * sections + 5),
        out_specs=memory,
        out_shape=jax.ShapeDtypeStruct((2, width, head), jnp.float32),
        scratch_shapes=[
            pltpu.VMEM((2, 2 * every, head), jnp.bfloat16),
            pltpu.VMEM((2 * every, width), jnp.bfloat16),
            pltpu.VMEM((2, every, (sections - 1) * head), jnp.bfloat16),
        ],
        name="weight_side",
        compiler_params=pltpu.CompilerParams(vmem_limit_bytes=20 << 20),
    )(
        place,
        *near_columns,
        *far_columns,
        *near_halves,
        *far_halves,
        near_mirror,
        far_mirror,
        *near_aside,
        *far_aside,
        *near_sent,
        *far_sent,
        own_slice,
        *fetched[1:],
        *lent[1:],
    )
    shape = (1, 2, seqs, length, model_width)
    return (grads_in.reshape(shape), weight_grads[None])


def shards(*operands):
    layer_inputs, held_weights = operands[0], operands[3]
    sections = lax.axis_size("section")
    replicas = lax.axis_size("dp")
    seqs, length, model_width = layer_inputs.shape[2:]
    head = held_weights.shape[-1]
    every_token = replicas * seqs * length
    moved = 2 * every_token * ((sections + 1) * head + 2 * model_width // replicas) * 2
    partial_sums = 4 * model_width * head * 4
    even = replicas % 2 == 0 and sections > 1 and sections & (sections - 1) == 0
    if even and moved < partial_sums and 2 * seqs * length <= head:
        return gathered(*operands)
    return reduced(*operands)


def solution(mesh):
    return jax.shard_map(
        shards,
        mesh=mesh,
        in_specs=(
            P("section", None, "dp", None, None),
            P("section", None, "dp", None, None),
            P("section", None, "dp", None, None),
            P("section", None, None, None, None),
            P(None, "dp", None, None),
            P(None, "dp"),
        ),
        out_specs=(P("section", None, "dp", None, None), P("section", None, "dp", None)),
        check_vma=False,
    )
```

```python
import functools
import math

import jax
import jax.numpy as jnp
from jax import lax
from jax.experimental import pallas as pl
from jax.experimental.pallas import tpu as pltpu
from jax.sharding import PartitionSpec as P


def passed_along(block, axis, distance):
    devices = range(lax.axis_size(axis))
    route = [(i - distance, i) for i in devices if i - distance in devices]
    return lax.ppermute(block, axis, route)


def from_partner(block, axis, bit):
    count = lax.axis_size(axis)
    route = []
    for low in range(count):
        high = low | 1 << bit
        if high != low and high < count:
            route += [(low, high), (high, low)]
    return lax.ppermute(block, axis, route)


def attention_weights(queries, key_vectors, valid_lengths):
    length = queries.shape[-2]
    scores = jnp.einsum(
        "nmth,nmsh->nmts", queries, key_vectors, preferred_element_type=jnp.float32
    ) / math.sqrt(queries.shape[-1])
    row_pos = lax.broadcasted_iota(jnp.int32, (length, length), 0)
    col_pos = lax.broadcasted_iota(jnp.int32, (length, length), 1)
    allowed = (col_pos <= row_pos)[None, None] & (
        col_pos[None, None] < valid_lengths[:, :, None, None]
    )
    scores = jnp.where(allowed, scores, -jnp.inf)
    row_max = jnp.max(scores, axis=-1, keepdims=True)
    raised = jnp.where(allowed, jnp.exp(scores - row_max), 0.0)
    return (raised / jnp.sum(raised, axis=-1, keepdims=True)).astype(jnp.bfloat16)


def reduced(layer_inputs, saved_queries, saved_keys, held_weights, cotangent, valid_lengths):
    sections = lax.axis_size("section")
    position = lax.axis_index("section")
    inputs = layer_inputs[0]
    value_w = held_weights[0, :, 0]
    output_w = held_weights[0, :, 1]
    attend = attention_weights(saved_queries[0], saved_keys[0], valid_lengths)
    micro_count = inputs.shape[1]
    length = inputs.shape[2]
    model_width = inputs.shape[3]
    head_size = value_w.shape[2]
    values = jnp.einsum(
        "nmld,ndh->nmlh", inputs, value_w, preferred_element_type=jnp.float32
    ).astype(jnp.bfloat16)
    mixtures = jnp.einsum(
        "nmts,nmsh->nmth", attend, values, preferred_element_type=jnp.float32
    ).astype(jnp.bfloat16)
    is_end = [position == sections - 1, position == 0]
    starts = [sections - 1 - position, position]

    def make_compute(direction):

        def compute(operands):
            grads, uppers, vgrads, incoming, index = operands
            fresh = lax.dynamic_index_in_dim(cotangent[direction], index, 0, keepdims=False)
            upstream = jnp.where(is_end[direction], fresh, incoming)
            weights_now = lax.dynamic_index_in_dim(attend[direction], index, 0, keepdims=False)
            out_grad = jnp.dot(
                upstream, output_w[direction], preferred_element_type=jnp.float32
            ).astype(jnp.bfloat16)
            val_grad = jnp.einsum(
                "ts,th->sh", weights_now, out_grad, preferred_element_type=jnp.float32
            ).astype(jnp.bfloat16)
            branch = jnp.einsum(
                "lh,dh->ld", val_grad, value_w[direction], preferred_element_type=jnp.float32
            )
            grad_input = (upstream.astype(jnp.float32) + branch).astype(jnp.bfloat16)
            grads = lax.dynamic_update_index_in_dim(grads, grad_input, index, 0)
            uppers = lax.dynamic_update_index_in_dim(uppers, upstream, index, 0)
            vgrads = lax.dynamic_update_index_in_dim(vgrads, val_grad, index, 0)
            return (grad_input, (grads, uppers, vgrads))

        return compute

    def skip(operands):
        grads, uppers, vgrads, incoming, _ = operands
        return (jnp.zeros_like(incoming), (grads, uppers, vgrads))

    def advance(moment, received, buffers):
        outgoing = []
        updated = []
        for direction in range(2):
            micro_id = moment - starts[direction]
            active = (micro_id >= 0) & (micro_id < micro_count)
            clipped = jnp.clip(micro_id, 0, micro_count - 1)
            grads, uppers, vgrads = buffers[direction]
            sent_now, fresh_buffers = lax.cond(
                active,
                make_compute(direction),
                skip,
                (grads, uppers, vgrads, received[direction], clipped),
            )
            outgoing.append(sent_now)
            updated.append(fresh_buffers)
        return (jnp.stack(outgoing), tuple(updated))

    big_zero = jnp.zeros((micro_count, length, model_width), jnp.bfloat16)
    small_zero = jnp.zeros((micro_count, length, head_size), jnp.bfloat16)
    buffers = ((big_zero, big_zero, small_zero), (big_zero, big_zero, small_zero))
    sent, buffers = advance(
        jnp.int32(0), jnp.zeros((2, length, model_width), jnp.bfloat16), buffers
    )

    def loop_body(moment, carried):
        outgoing, held = carried
        from_next = passed_along(outgoing[0], "section", -1)
        from_prev = passed_along(outgoing[1], "section", 1)
        return advance(moment, jnp.stack([from_next, from_prev]), held)

    sent, buffers = lax.fori_loop(1, sections + micro_count - 1, loop_body, (sent, buffers))
    grads_in = jnp.stack([buffers[0][0], buffers[1][0]])
    upstreams = jnp.stack([buffers[0][1], buffers[1][1]])
    val_grads = jnp.stack([buffers[0][2], buffers[1][2]])
    flat_in = inputs.reshape(2, micro_count * length, model_width)
    flat_up = upstreams.reshape(2, micro_count * length, model_width)
    flat_mix = mixtures.reshape(2, micro_count * length, head_size)
    flat_vg = val_grads.reshape(2, micro_count * length, head_size)
    grad_value = jnp.einsum("ntd,nth->dnh", flat_in, flat_vg, preferred_element_type=jnp.float32)
    grad_output = jnp.einsum("ntd,nth->dnh", flat_up, flat_mix, preferred_element_type=jnp.float32)
    summed = lax.psum_scatter(
        jnp.stack([grad_value, grad_output], axis=2).reshape(
            model_width // lax.axis_size("dp") * lax.axis_size("dp"), 4 * head_size
        ),
        "dp",
        scatter_dimension=0,
        tiled=True,
    )
    summed = summed.reshape(-1, 2, 2, head_size)
    own_part = summed[:, 0]
    mirror_part = summed[:, 1]
    for bit_no in range(sections.bit_length() - 1):
        mirror_part = from_partner(mirror_part.astype(jnp.bfloat16), "section", bit_no).astype(
            mirror_part.dtype
        )
    combined = own_part + mirror_part
    weight_grads = jnp.transpose(combined, (1, 0, 2))[None]
    return (grads_in[None], weight_grads)


def swapped(block, axis, mask):
    return lax.ppermute(block, axis, [(i, i ^ mask) for i in range(lax.axis_size(axis))])


def shifted(block, distance):
    count = lax.axis_size("dp")
    return lax.ppermute(block, "dp", [(i, (i + 2 * distance) % count) for i in range(count)])


def contract(left, right, left_dim, right_dim):
    return lax.dot_general(
        left, right, (((left_dim,), (right_dim,)), ((), ())), preferred_element_type=jnp.float32
    )


def heads_kernel(length, valid, inputs, cot, held, queries, key_vectors, short, out, sums):
    tokens, head = queries.shape[1:]
    for way in range(2):
        for which, source in enumerate((inputs, cot)):
            term = contract(source[way], held[way, which], 1, 0)
            first = pl.program_id(0) == 0

            @pl.when(first)
            def _():
                sums[which, way] = term

            @pl.when(jnp.logical_not(first))
            def _():
                sums[which, way] += term

    @pl.when(pl.program_id(0) == pl.num_programs(0) - 1)
    def _():
        row = lax.broadcasted_iota(jnp.int32, (tokens, tokens), 0)
        col = lax.broadcasted_iota(jnp.int32, (tokens, tokens), 1)
        out[2 * tokens : 3 * tokens, :] = jnp.zeros((tokens, head), jnp.bfloat16)
        for way in range(2):
            scores = contract(queries[way], key_vectors[way], 1, 1) / math.sqrt(head)
            allowed = None
            for seq in range(tokens // length):
                start = seq * length
                here = (row >= start) & (row < start + length) & (col >= start) & (col <= row)
                here &= col - start < valid[way, seq]
                allowed = here if allowed is None else allowed | here
            scores = jnp.where(allowed, scores, -jnp.inf)
            row_max = jnp.max(scores, axis=-1, keepdims=True)
            raised = jnp.where(allowed, jnp.exp(scores - row_max), 0.0)
            attend = (raised / jnp.sum(raised, axis=-1, keepdims=True)).astype(jnp.bfloat16)
            mixture = contract(attend, sums[0, way].astype(jnp.bfloat16), 1, 0)
            out[way * tokens : (way + 1) * tokens, :] = sums[1, way].astype(jnp.bfloat16)
            out[2 * tokens : 3 * tokens, way * tokens : (way + 1) * tokens] = attend
            rows = slice((3 + way) * tokens, (4 + way) * tokens)
            out[rows, :] = mixture.astype(jnp.bfloat16)
        short[...] = out[: 3 * tokens, :]


def pack_kernel(near, far, out):
    out[...] = (near[...] + far[...]).astype(jnp.bfloat16)


def chain_kernel(sections, tokens, head, *refs):
    place = position()
    parts, tails = refs[:sections], refs[sections : 2 * sections]
    gathered, steer, own = refs[2 * sections :]

    def at(here):
        mine = [[None] * sections, [None] * sections]
        for way in range(2):
            order = range(sections - 1, -1, -1) if way == 0 else range(sections)
            done = []
            for holder in order:
                part, tail = parts[here ^ holder], tails[here ^ holder]
                total = tail[way * tokens : (way + 1) * tokens, :].astype(jnp.float32)
                for other in done:
                    total += contract(mine[way][other], part[(other ^ holder) - 1], 1, 0)
                weights = tail[2 * tokens : 3 * tokens, way * tokens : (way + 1) * tokens]
                mine[way][holder] = contract(weights, total.astype(jnp.bfloat16), 0, 0).astype(
                    jnp.bfloat16
                )
                done.append(holder)
        zero = jnp.zeros((tokens, head), jnp.bfloat16)
        for far in range(sections):
            inside = here + far < sections
            gathered[0, far] = mine[0][here + far] if inside else zero
            gathered[1, far] = mine[1][sections - 1 - here - far] if inside else zero
        mirror = here ^ (sections - 1)
        gathered[0, sections] = tails[0][3 * tokens : 4 * tokens, :]
        gathered[1, sections] = tails[here ^ mirror][4 * tokens : 5 * tokens, :]
        for way in range(2):
            own[way] = mine[way][here]
        for mask in range(1, sections):
            other = here ^ mask
            way = 0 if other > here else 1
            lanes = slice((mask - 1) * head, mask * head)
            steer[way * tokens : (way + 1) * tokens, lanes] = mine[way][other]
            steer[(1 - way) * tokens : (2 - way) * tokens, lanes] = zero

    for here in range(sections):

        @pl.when(place[0] == here)
        def _():
            at(here)


def input_kernel(sections, tokens, cot, steer, own, held, *refs):
    place = position()
    near, far = refs[: sections - 1], refs[sections - 1 : 2 * sections - 2]
    out = refs[2 * sections - 2]
    width = near[0].shape[1]
    core = place[1]
    for which, fetched in ((core, near), (1 - core, far)):
        start = pl.multiple_of(which * width, 128)
        weights = jnp.concatenate([block[0] for block in fetched], axis=1)
        total = contract(steer[...], weights, 1, 1)
        for way in range(2):
            branch = contract(own[way], held[way, pl.ds(start, width), :], 1, 1)
            branch += total[way * tokens : (way + 1) * tokens]
            base = cot[way, :, pl.ds(start, width)].astype(jnp.float32)
            out[way, :, pl.ds(start, width)] = (base + branch).astype(jnp.bfloat16)


def pick_weights(sections, halved, *refs):
    place = position()
    outs, sems = refs[: sections - 1], refs[sections - 1]
    here, core = place[0], place[1]
    copies = []
    for mask in range(sections - 1, 0, -1):
        way = jnp.where((here ^ mask) < here, 0, 1)
        copy = pltpu.make_async_copy(
            halved.at[way, 0, :, core], outs[mask - 1], sems.at[mask - 1]
        )
        copy.start()
        copies.append(copy)
    for copy in copies:
        copy.wait()


def position():
    here, replica = lax.axis_index("section"), lax.axis_index("dp")
    asides = (lax.axis_size("section") // 2, 1)
    bits = [jnp.where((here & aside) != 0, 1, 0) for aside in asides]
    return (here, lax.rem(replica, 2), lax.div(replica, 2), *bits)


def carried_out(copies):
    for copy in copies:
        copy.start()
    for copy in copies:
        copy.wait()


def pick_outputs(halved, whole, out, own, part, sems):
    place = position()
    carried_out(
        [
            pltpu.make_async_copy(halved.at[1, 0, place[2], place[1]], part, sems.at[2]),
            pltpu.make_async_copy(halved.at[:, 1, :, place[1]], out, sems.at[0]),
            pltpu.make_async_copy(whole.at[:, 0], own, sems.at[1]),
        ]
    )


def pick_columns(steps, width, inputs, cot, *refs):
    place = position()
    outs, halves, sems = refs[:steps], refs[steps : 2 * steps], refs[2 * steps]
    copies = []
    for distance in range(steps):
        start = pl.multiple_of((place[2] + distance) % steps * 2 * width, 128)
        copies.append(
            pltpu.make_async_copy(
                inputs.at[:, :, pl.ds(start, 2 * width)], outs[distance], sems.at[3 * distance]
            )
        )
        for way in range(2):
            half = pl.multiple_of(start + place[3 + way] * width, 128)
            copies.append(
                pltpu.make_async_copy(
                    cot.at[way, :, pl.ds(half, width)],
                    halves[distance].at[way],
                    sems.at[3 * distance + 1 + way],
                )
            )
    carried_out(copies)


def pick_moving(steps, which, *refs):
    sources, outs, sems = refs[:steps], refs[steps:-1], refs[-1]
    copies = []
    for step, source in enumerate(sources):
        for index, out in zip(which, outs):
            copies.append(
                pltpu.make_async_copy(source.at[index], out.at[step], sems.at[len(copies)])
            )
    carried_out(copies)


def product_kernel(sections, steps, outputs, *refs):
    place = position()
    fetched, out = refs[: sections - 1], refs[sections - 1]
    for mask in range(1, sections):
        way = jnp.where((place[0] ^ mask) > place[0], 0, 1)
        total = None
        for step in range(steps):
            term = contract(fetched[mask - 1][step], outputs[way, step], 0, 0)
            total = term if total is None else total + term
        out[mask - 1] = total


def weight_kernel(sections, steps, tokens, *refs):
    place = position()
    columns = refs[: 2 * steps]
    halves, refs = refs[2 * steps : 4 * steps], refs[2 * steps :]
    mirrored, lent = refs[2 * steps : 2 * steps + 2], refs[2 * steps + 2 : 2 * steps + 6]
    sent = refs[2 * steps + 6 : 4 * steps + 6]
    refs = refs[4 * steps + 6 :]
    own_slice, fetched, lent_slices = refs[0], refs[:sections], refs[sections - 1 :]
    out, lefts, rights, steers = refs[2 * sections - 1 :]
    width, head = out.shape[1:]
    every = 2 * steps * tokens
    lanes = pl.ds(pl.multiple_of(place[1] * width, 128), width)
    for index in range(2 * steps):
        rows = slice(index * tokens, (index + 1) * tokens)
        for way in range(2):
            for far in range(1, sections):
                steers[way, rows, (far - 1) * head : far * head] = sent[index][way, far]
            both = slice(way * every + index * tokens, way * every + (index + 1) * tokens)
            lefts[0, both, :] = sent[index][way, 0]
            lefts[1, both, :] = sent[index][way, sections]
        rights[rows, :] = columns[index][0, :, lanes]
        rows = slice(every + index * tokens, every + (index + 1) * tokens)
        rights[rows, :] = mirrored[index // steps][index % steps, :, lanes]
    out[0] = contract(lefts[0], rights[...], 0, 0).T
    for index in range(2 * steps):
        for way in range(2):
            both = slice(way * every + index * tokens, way * every + (index + 1) * tokens)

            @pl.when(place[3 + way] == place[1])
            def _():
                rights[both, :] = halves[index][way]

            @pl.when(place[3 + way] != place[1])
            def _():
                rights[both, :] = lent[2 * (index // steps) + way][index % steps]

    def corrected(here, way):
        rows = slice(way * every, (way + 1) * every)
        blocks = []
        for far in range(1, sections - here):
            holder = here + far if way == 0 else sections - 1 - here - far
            if holder == here:
                blocks.append(own_slice[...])
            elif way == 1 and holder > here:
                blocks.append(lent_slices[holder ^ here][...])
            else:
                blocks.append(fetched[holder ^ here][place[2]])
        steer = steers[way, :, : len(blocks) * head]
        total = contract(steer, jnp.concatenate(blocks, axis=1), 1, 1)
        rights[rows, :] = (rights[rows, :].astype(jnp.float32) + total).astype(jnp.bfloat16)

    for here in range(sections - 1):

        @pl.when(place[0] == here)
        def _():
            for way in range(2):
                corrected(here, way)

    out[1] = contract(lefts[1], rights[...], 0, 0).T


def gathered(layer_inputs, saved_queries, saved_keys, held_weights, cotangent, valid_lengths):
    sections = lax.axis_size("section")
    replicas = lax.axis_size("dp")
    steps = replicas // 2
    inputs = layer_inputs[0]
    held = held_weights[0]
    seqs, length, model_width = inputs.shape[1:]
    tokens = seqs * length
    head = held.shape[-1]
    width = model_width // replicas
    inputs = inputs.reshape(2, tokens, model_width)
    cot = cotangent.reshape(2, tokens, model_width)
    halved = held.reshape(2, 2, steps, 2, width, head)
    asides = (sections // 2, 1)
    memory = pl.BlockSpec(memory_space=pltpu.VMEM)
    scalars = pl.BlockSpec(memory_space=pltpu.SMEM)
    anywhere = pl.BlockSpec(memory_space=pl.ANY)
    hbm = pl.BlockSpec(memory_space=pltpu.HBM)

    picked = pl.pallas_call(
        functools.partial(pick_weights, sections),
        in_specs=[hbm],
        out_specs=[memory] * (sections - 1),
        out_shape=[jax.ShapeDtypeStruct((steps, width, head), jnp.bfloat16)] * (sections - 1),
        scratch_shapes=[pltpu.SemaphoreType.DMA((sections - 1,))],
        name="pick_weights",
        compiler_params=pltpu.CompilerParams(vmem_limit_bytes=52 << 20),
    )(halved)
    fetched = [None] * sections
    for mask in range(sections - 1, 0, -1):
        fetched[mask] = swapped(picked[mask - 1], "section", mask)

    wide = jax.ShapeDtypeStruct((2, tokens, 2 * width), jnp.bfloat16)
    slim = jax.ShapeDtypeStruct((2, tokens, width), jnp.bfloat16)
    picked = pl.pallas_call(
        functools.partial(pick_columns, steps, width),
        in_specs=[hbm] * 2,
        out_specs=[memory] * (2 * steps),
        out_shape=[wide] * steps + [slim] * steps,
        scratch_shapes=[pltpu.SemaphoreType.DMA((3 * steps,))],
        name="pick_columns",
        compiler_params=pltpu.CompilerParams(vmem_limit_bytes=52 << 20),
    )(inputs, cot)
    near_columns, near_halves = [picked[0]], [picked[steps]]
    for distance in range(1, steps):
        near_halves.append(shifted(picked[steps + distance], distance))
    for distance in range(1, steps):
        near_columns.append(shifted(picked[distance], distance))

    def moving(sources, which, shape):
        return pl.pallas_call(
            functools.partial(pick_moving, steps, which),
            in_specs=[anywhere] * steps,
            out_specs=[memory] * len(which),
            out_shape=[jax.ShapeDtypeStruct((steps,) + shape, jnp.bfloat16)] * len(which),
            scratch_shapes=[pltpu.SemaphoreType.DMA((steps * len(which),))],
            name="pick_moving",
            compiler_params=pltpu.CompilerParams(vmem_limit_bytes=8 << 20),
        )(*sources)

    sideways = moving(near_halves, (0, 1), (tokens, width))
    near_aside, far_aside, far_columns, far_halves = [], [], [], []
    for way in range(2):
        near_aside.append(swapped(sideways[way], "section", asides[way]))
    for way in range(2):
        far_aside.append(swapped(near_aside[way], "dp", 1))
    for distance in range(steps):
        far_halves.append(swapped(near_halves[distance], "dp", 1))

    lengths = valid_lengths
    blocks = 4
    cut = model_width // blocks
    short, full = pl.pallas_call(
        functools.partial(heads_kernel, length),
        grid=(blocks,),
        in_specs=[
            scalars,
            pl.BlockSpec((2, tokens, cut), lambda i: (0, 0, i)),
            pl.BlockSpec((2, tokens, cut), lambda i: (0, 0, i)),
            pl.BlockSpec((2, 2, cut, head), lambda i: (0, 0, i, 0)),
            pl.BlockSpec((2, tokens, head), lambda i: (0, 0, 0)),
            pl.BlockSpec((2, tokens, head), lambda i: (0, 0, 0)),
        ],
        out_specs=[pl.BlockSpec((rows * tokens, head), lambda i: (0, 0)) for rows in (3, 5)],
        out_shape=[jax.ShapeDtypeStruct((rows * tokens, head), jnp.bfloat16) for rows in (3, 5)],
        scratch_shapes=[pltpu.VMEM((2, 2, tokens, head), jnp.float32)],
        name="heads",
        compiler_params=pltpu.CompilerParams(vmem_limit_bytes=12 << 20),
    )(
        lengths,
        inputs,
        cot,
        held,
        saved_queries[0].reshape(2, tokens, head),
        saved_keys[0].reshape(2, tokens, head),
    )

    tails = [full]
    for mask in range(1, sections):
        tails.append(swapped(full if mask == sections - 1 else short, "section", mask))

    outputs, own_values, own_slice = pl.pallas_call(
        pick_outputs,
        in_specs=[hbm, hbm],
        out_specs=[memory] * 3,
        out_shape=[
            jax.ShapeDtypeStruct((2, steps, width, head), jnp.bfloat16),
            jax.ShapeDtypeStruct((2, model_width, head), jnp.bfloat16),
            jax.ShapeDtypeStruct((width, head), jnp.bfloat16),
        ],
        scratch_shapes=[pltpu.SemaphoreType.DMA((3,))],
        name="pick_outputs",
        compiler_params=pltpu.CompilerParams(vmem_limit_bytes=8 << 20),
    )(halved, held)
    products = pl.pallas_call(
        functools.partial(product_kernel, sections, steps),
        in_specs=[memory] * sections,
        out_specs=memory,
        out_shape=jax.ShapeDtypeStruct((sections - 1, head, head), jnp.float32),
        name="products",
        compiler_params=pltpu.CompilerParams(vmem_limit_bytes=8 << 20),
    )(outputs, *fetched[1:])
    far_products = swapped(products, "dp", 1)
    lent_back = [None] * sections
    for mask in range(1, sections):
        lent_back[mask] = swapped(fetched[mask], "dp", 1)

    packed = pl.pallas_call(
        pack_kernel,
        in_specs=[memory] * 2,
        out_specs=memory,
        out_shape=jax.ShapeDtypeStruct((sections - 1, head, head), jnp.bfloat16),
        name="pack",
        compiler_params=pltpu.CompilerParams(vmem_limit_bytes=8 << 20),
    )(products, far_products)
    parts = [packed]
    for mask in range(1, sections):
        parts.append(swapped(packed, "section", mask))

    (upward,) = moving(near_columns, (1,), (tokens, 2 * width))
    near_mirror = swapped(upward, "section", sections - 1)
    far_mirror = swapped(near_mirror, "dp", 1)
    for distance in range(steps):
        far_columns.append(swapped(near_columns[distance], "dp", 1))
    lent = [own_slice]
    for mask in range(1, sections):
        route = [
            (i, i ^ mask) for i in range(sections) if i ^ mask < i < sections - 1 - (i ^ mask)
        ]
        lent.append(lax.ppermute(own_slice, "section", route) if route else own_slice)

    sent, steer, own = pl.pallas_call(
        functools.partial(chain_kernel, sections, tokens, head),
        in_specs=[memory] * (2 * sections),
        out_specs=(memory, memory, memory),
        out_shape=(
            jax.ShapeDtypeStruct((2, sections + 1, tokens, head), jnp.bfloat16),
            jax.ShapeDtypeStruct((2 * tokens, (sections - 1) * head), jnp.bfloat16),
            jax.ShapeDtypeStruct((2, tokens, head), jnp.bfloat16),
        ),
        name="chain",
        compiler_params=pltpu.CompilerParams(vmem_limit_bytes=8 << 20),
    )(*parts, *tails)

    near_sent = [sent]
    for distance in range(1, steps):
        near_sent.append(shifted(sent, distance))
    far_sent = []
    for distance in range(steps):
        far_sent.append(swapped(near_sent[distance], "dp", 1))

    grads_in = pl.pallas_call(
        functools.partial(input_kernel, sections, tokens),
        grid=(steps,),
        in_specs=[
            pl.BlockSpec((2, tokens, 2 * width), lambda i: (0, 0, i)),
            pl.BlockSpec((2 * tokens, (sections - 1) * head), lambda i: (0, 0)),
            pl.BlockSpec((2, tokens, head), lambda i: (0, 0, 0)),
            pl.BlockSpec((2, 2 * width, head), lambda i: (0, i, 0)),
        ]
        + [pl.BlockSpec((1, width, head), lambda i: (i, 0, 0))] * (2 * sections - 2),
        out_specs=pl.BlockSpec((2, tokens, 2 * width), lambda i: (0, 0, i)),
        out_shape=jax.ShapeDtypeStruct((2, tokens, model_width), jnp.bfloat16),
        name="input_side",
        compiler_params=pltpu.CompilerParams(vmem_limit_bytes=12 << 20),
    )(cot, steer, own, own_values, *fetched[1:], *lent_back[1:])

    every = replicas * tokens
    weight_grads = pl.pallas_call(
        functools.partial(weight_kernel, sections, steps, tokens),
        in_specs=[memory] * (6 * steps + 2 * sections + 5),
        out_specs=memory,
        out_shape=jax.ShapeDtypeStruct((2, width, head), jnp.float32),
        scratch_shapes=[
            pltpu.VMEM((2, 2 * every, head), jnp.bfloat16),
            pltpu.VMEM((2 * every, width), jnp.bfloat16),
            pltpu.VMEM((2, every, (sections - 1) * head), jnp.bfloat16),
        ],
        name="weight_side",
        compiler_params=pltpu.CompilerParams(vmem_limit_bytes=20 << 20),
    )(
        *near_columns,
        *far_columns,
        *near_halves,
        *far_halves,
        near_mirror,
        far_mirror,
        *near_aside,
        *far_aside,
        *near_sent,
        *far_sent,
        own_slice,
        *fetched[1:],
        *lent[1:],
    )
    shape = (1, 2, seqs, length, model_width)
    return (grads_in.reshape(shape), weight_grads[None])


def shards(*operands):
    layer_inputs, held_weights = operands[0], operands[3]
    sections = lax.axis_size("section")
    replicas = lax.axis_size("dp")
    seqs, length, model_width = layer_inputs.shape[2:]
    head = held_weights.shape[-1]
    every_token = replicas * seqs * length
    moved = 2 * every_token * ((sections + 1) * head + 2 * model_width // replicas) * 2
    partial_sums = 4 * model_width * head * 4
    even = replicas % 2 == 0 and sections > 1 and sections & (sections - 1) == 0
    if even and moved < partial_sums and 2 * seqs * length <= head:
        return gathered(*operands)
    return reduced(*operands)


def solution(mesh):
    return jax.shard_map(
        shards,
        mesh=mesh,
        in_specs=(
            P("section", None, "dp", None, None),
            P("section", None, "dp", None, None),
            P("section", None, "dp", None, None),
            P("section", None, None, None, None),
            P(None, "dp", None, None),
            P(None, "dp"),
        ),
        out_specs=(P("section", None, "dp", None, None), P("section", None, "dp", None)),
        check_vma=False,
    )
```

```python
import functools
import math

import jax
import jax.numpy as jnp
from jax import lax
from jax.experimental import pallas as pl
from jax.experimental.pallas import tpu as pltpu
from jax.sharding import PartitionSpec as P


SECTION = "section"


def passed_along(block, axis, distance):
    devices = range(lax.axis_size(axis))
    route = [(i - distance, i) for i in devices if i - distance in devices]
    return lax.ppermute(block, axis, route)


def from_partner(block, axis, bit):
    count = lax.axis_size(axis)
    route = []
    for low in range(count):
        high = low | 1 << bit
        if high != low and high < count:
            route += [(low, high), (high, low)]
    return lax.ppermute(block, axis, route)


def attention_weights(queries, key_vectors, valid_lengths):
    length = queries.shape[-2]
    scores = jnp.einsum(
        "nmth,nmsh->nmts", queries, key_vectors, preferred_element_type=jnp.float32
    ) / math.sqrt(queries.shape[-1])
    row_pos = lax.broadcasted_iota(jnp.int32, (length, length), 0)
    col_pos = lax.broadcasted_iota(jnp.int32, (length, length), 1)
    allowed = (col_pos <= row_pos)[None, None] & (
        col_pos[None, None] < valid_lengths[:, :, None, None]
    )
    scores = jnp.where(allowed, scores, -jnp.inf)
    row_max = jnp.max(scores, axis=-1, keepdims=True)
    raised = jnp.where(allowed, jnp.exp(scores - row_max), 0.0)
    return (raised / jnp.sum(raised, axis=-1, keepdims=True)).astype(jnp.bfloat16)


def reduced(layer_inputs, saved_queries, saved_keys, held_weights, cotangent, valid_lengths):
    sections = lax.axis_size(SECTION)
    position = lax.axis_index(SECTION)
    inputs = layer_inputs[0]
    value_w = held_weights[0, :, 0]
    output_w = held_weights[0, :, 1]
    attend = attention_weights(saved_queries[0], saved_keys[0], valid_lengths)
    micro_count = inputs.shape[1]
    length = inputs.shape[2]
    model_width = inputs.shape[3]
    head_size = value_w.shape[2]
    values = jnp.einsum(
        "nmld,ndh->nmlh", inputs, value_w, preferred_element_type=jnp.float32
    ).astype(jnp.bfloat16)
    mixtures = jnp.einsum(
        "nmts,nmsh->nmth", attend, values, preferred_element_type=jnp.float32
    ).astype(jnp.bfloat16)
    is_end = [position == sections - 1, position == 0]
    starts = [sections - 1 - position, position]

    def make_compute(direction):

        def compute(operands):
            grads, uppers, vgrads, incoming, index = operands
            fresh = lax.dynamic_index_in_dim(cotangent[direction], index, 0, keepdims=False)
            upstream = jnp.where(is_end[direction], fresh, incoming)
            weights_now = lax.dynamic_index_in_dim(attend[direction], index, 0, keepdims=False)
            out_grad = jnp.dot(
                upstream, output_w[direction], preferred_element_type=jnp.float32
            ).astype(jnp.bfloat16)
            val_grad = jnp.einsum(
                "ts,th->sh", weights_now, out_grad, preferred_element_type=jnp.float32
            ).astype(jnp.bfloat16)
            branch = jnp.einsum(
                "lh,dh->ld", val_grad, value_w[direction], preferred_element_type=jnp.float32
            )
            grad_input = (upstream.astype(jnp.float32) + branch).astype(jnp.bfloat16)
            grads = lax.dynamic_update_index_in_dim(grads, grad_input, index, 0)
            uppers = lax.dynamic_update_index_in_dim(uppers, upstream, index, 0)
            vgrads = lax.dynamic_update_index_in_dim(vgrads, val_grad, index, 0)
            return (grad_input, (grads, uppers, vgrads))

        return compute

    def skip(operands):
        grads, uppers, vgrads, incoming, _ = operands
        return (jnp.zeros_like(incoming), (grads, uppers, vgrads))

    def advance(moment, received, buffers):
        outgoing = []
        updated = []
        for direction in range(2):
            micro_id = moment - starts[direction]
            active = (micro_id >= 0) & (micro_id < micro_count)
            clipped = jnp.clip(micro_id, 0, micro_count - 1)
            grads, uppers, vgrads = buffers[direction]
            sent_now, fresh_buffers = lax.cond(
                active,
                make_compute(direction),
                skip,
                (grads, uppers, vgrads, received[direction], clipped),
            )
            outgoing.append(sent_now)
            updated.append(fresh_buffers)
        return (jnp.stack(outgoing), tuple(updated))

    big_zero = jnp.zeros((micro_count, length, model_width), jnp.bfloat16)
    small_zero = jnp.zeros((micro_count, length, head_size), jnp.bfloat16)
    buffers = ((big_zero, big_zero, small_zero), (big_zero, big_zero, small_zero))
    sent, buffers = advance(
        jnp.int32(0), jnp.zeros((2, length, model_width), jnp.bfloat16), buffers
    )

    def loop_body(moment, carried):
        outgoing, held = carried
        from_next = passed_along(outgoing[0], SECTION, -1)
        from_prev = passed_along(outgoing[1], SECTION, 1)
        return advance(moment, jnp.stack([from_next, from_prev]), held)

    sent, buffers = lax.fori_loop(1, sections + micro_count - 1, loop_body, (sent, buffers))
    grads_in = jnp.stack([buffers[0][0], buffers[1][0]])
    upstreams = jnp.stack([buffers[0][1], buffers[1][1]])
    val_grads = jnp.stack([buffers[0][2], buffers[1][2]])
    flat_in = inputs.reshape(2, micro_count * length, model_width)
    flat_up = upstreams.reshape(2, micro_count * length, model_width)
    flat_mix = mixtures.reshape(2, micro_count * length, head_size)
    flat_vg = val_grads.reshape(2, micro_count * length, head_size)
    grad_value = jnp.einsum("ntd,nth->dnh", flat_in, flat_vg, preferred_element_type=jnp.float32)
    grad_output = jnp.einsum("ntd,nth->dnh", flat_up, flat_mix, preferred_element_type=jnp.float32)
    summed = lax.psum_scatter(
        jnp.stack([grad_value, grad_output], axis=2).reshape(
            model_width // lax.axis_size("dp") * lax.axis_size("dp"), 4 * head_size
        ),
        "dp",
        scatter_dimension=0,
        tiled=True,
    )
    summed = summed.reshape(-1, 2, 2, head_size)
    own_part = summed[:, 0]
    mirror_part = summed[:, 1]
    for bit_no in range(sections.bit_length() - 1):
        mirror_part = from_partner(mirror_part.astype(jnp.bfloat16), SECTION, bit_no).astype(
            mirror_part.dtype
        )
    combined = own_part + mirror_part
    weight_grads = jnp.transpose(combined, (1, 0, 2))[None]
    return (grads_in[None], weight_grads)


def swapped(block, axis, mask):
    return lax.ppermute(block, axis, [(i, i ^ mask) for i in range(lax.axis_size(axis))])


def shifted(block, distance):
    count = lax.axis_size("dp")
    return lax.ppermute(block, "dp", [(i, (i + 2 * distance) % count) for i in range(count)])


def contract(left, right, left_dim, right_dim):
    return lax.dot_general(
        left, right, (((left_dim,), (right_dim,)), ((), ())), preferred_element_type=jnp.float32
    )


def heads_kernel(length, valid, inputs, cot, held, queries, key_vectors, short, out, sums):
    tokens, head = queries.shape[1:]
    for way in range(2):
        for which, source in enumerate((inputs, cot)):
            term = contract(source[way], held[way, which], 1, 0)
            first = pl.program_id(0) == 0

            @pl.when(first)
            def _():
                sums[which, way] = term

            @pl.when(jnp.logical_not(first))
            def _():
                sums[which, way] += term

    @pl.when(pl.program_id(0) == pl.num_programs(0) - 1)
    def _():
        row = lax.broadcasted_iota(jnp.int32, (tokens, tokens), 0)
        col = lax.broadcasted_iota(jnp.int32, (tokens, tokens), 1)
        out[2 * tokens : 3 * tokens, :] = jnp.zeros((tokens, head), jnp.bfloat16)
        for way in range(2):
            scores = contract(queries[way], key_vectors[way], 1, 1) / math.sqrt(head)
            allowed = None
            for seq in range(tokens // length):
                start = seq * length
                here = (row >= start) & (row < start + length) & (col >= start) & (col <= row)
                here &= col - start < valid[way, seq]
                allowed = here if allowed is None else allowed | here
            scores = jnp.where(allowed, scores, -jnp.inf)
            row_max = jnp.max(scores, axis=-1, keepdims=True)
            raised = jnp.where(allowed, jnp.exp(scores - row_max), 0.0)
            attend = (raised / jnp.sum(raised, axis=-1, keepdims=True)).astype(jnp.bfloat16)
            mixture = contract(attend, sums[0, way].astype(jnp.bfloat16), 1, 0)
            out[way * tokens : (way + 1) * tokens, :] = sums[1, way].astype(jnp.bfloat16)
            out[2 * tokens : 3 * tokens, way * tokens : (way + 1) * tokens] = attend
            rows = slice((3 + way) * tokens, (4 + way) * tokens)
            out[rows, :] = mixture.astype(jnp.bfloat16)
        short[...] = out[: 3 * tokens, :]


def pack_kernel(near, far, out):
    out[...] = (near[...] + far[...]).astype(jnp.bfloat16)


def chain_kernel(sections, tokens, head, *refs):
    place = position()
    parts, tails = refs[:sections], refs[sections : 2 * sections]
    gathered, steer, own = refs[2 * sections :]

    def at(here):
        mine = [[None] * sections, [None] * sections]
        for way in range(2):
            order = range(sections - 1, -1, -1) if way == 0 else range(sections)
            done = []
            for holder in order:
                part, tail = parts[here ^ holder], tails[here ^ holder]
                total = tail[way * tokens : (way + 1) * tokens, :].astype(jnp.float32)
                for other in done:
                    total += contract(mine[way][other], part[(other ^ holder) - 1], 1, 0)
                weights = tail[2 * tokens : 3 * tokens, way * tokens : (way + 1) * tokens]
                mine[way][holder] = contract(weights, total.astype(jnp.bfloat16), 0, 0).astype(
                    jnp.bfloat16
                )
                done.append(holder)
        zero = jnp.zeros((tokens, head), jnp.bfloat16)
        for far in range(sections):
            inside = here + far < sections
            gathered[0, far] = mine[0][here + far] if inside else zero
            gathered[1, far] = mine[1][sections - 1 - here - far] if inside else zero
        mirror = here ^ (sections - 1)
        gathered[0, sections] = tails[0][3 * tokens : 4 * tokens, :]
        gathered[1, sections] = tails[here ^ mirror][4 * tokens : 5 * tokens, :]
        for way in range(2):
            own[way] = mine[way][here]
        for mask in range(1, sections):
            other = here ^ mask
            way = 0 if other > here else 1
            lanes = slice((mask - 1) * head, mask * head)
            steer[way * tokens : (way + 1) * tokens, lanes] = mine[way][other]
            steer[(1 - way) * tokens : (2 - way) * tokens, lanes] = zero

    for here in range(sections):

        @pl.when(place[0] == here)
        def _():
            at(here)


def input_kernel(sections, tokens, cot, steer, own, held, *refs):
    place = position()
    near, far = refs[: sections - 1], refs[sections - 1 : 2 * sections - 2]
    out = refs[2 * sections - 2]
    width = near[0].shape[1]
    core = place[1]
    for which, fetched in ((core, near), (1 - core, far)):
        start = pl.multiple_of(which * width, 128)
        weights = jnp.concatenate([block[0] for block in fetched], axis=1)
        total = contract(steer[...], weights, 1, 1)
        for way in range(2):
            branch = contract(own[way], held[way, pl.ds(start, width), :], 1, 1)
            branch += total[way * tokens : (way + 1) * tokens]
            base = cot[way, :, pl.ds(start, width)].astype(jnp.float32)
            out[way, :, pl.ds(start, width)] = (base + branch).astype(jnp.bfloat16)


def pick_weights(sections, halved, *refs):
    place = position()
    outs, sems = refs[: sections - 1], refs[sections - 1]
    here, core = place[0], place[1]
    copies = []
    for mask in range(sections - 1, 0, -1):
        way = jnp.where((here ^ mask) < here, 0, 1)
        copy = pltpu.make_async_copy(
            halved.at[way, 0, :, core], outs[mask - 1], sems.at[mask - 1]
        )
        copy.start()
        copies.append(copy)
    for copy in copies:
        copy.wait()


def position():
    here, replica = lax.axis_index(SECTION), lax.axis_index("dp")
    asides = (lax.axis_size(SECTION) // 2, 1)
    bits = [jnp.where((here & aside) != 0, 1, 0) for aside in asides]
    return (here, lax.rem(replica, 2), lax.div(replica, 2), *bits)


def carried_out(copies):
    for copy in copies:
        copy.start()
    for copy in copies:
        copy.wait()


def pick_outputs(halved, whole, out, own, part, sems):
    place = position()
    carried_out(
        [
            pltpu.make_async_copy(halved.at[1, 0, place[2], place[1]], part, sems.at[2]),
            pltpu.make_async_copy(halved.at[:, 1, :, place[1]], out, sems.at[0]),
            pltpu.make_async_copy(whole.at[:, 0], own, sems.at[1]),
        ]
    )


def pick_columns(steps, width, inputs, cot, *refs):
    place = position()
    outs, halves, sems = refs[:steps], refs[steps : 2 * steps], refs[2 * steps]
    copies = []
    for distance in range(steps):
        start = pl.multiple_of((place[2] + distance) % steps * 2 * width, 128)
        copies.append(
            pltpu.make_async_copy(
                inputs.at[:, :, pl.ds(start, 2 * width)], outs[distance], sems.at[3 * distance]
            )
        )
        for way in range(2):
            half = pl.multiple_of(start + place[3 + way] * width, 128)
            copies.append(
                pltpu.make_async_copy(
                    cot.at[way, :, pl.ds(half, width)],
                    halves[distance].at[way],
                    sems.at[3 * distance + 1 + way],
                )
            )
    carried_out(copies)


def pick_moving(steps, which, *refs):
    sources, outs, sems = refs[:steps], refs[steps:-1], refs[-1]
    copies = []
    for step, source in enumerate(sources):
        for index, out in zip(which, outs):
            copies.append(
                pltpu.make_async_copy(source.at[index], out.at[step], sems.at[len(copies)])
            )
    carried_out(copies)


def product_kernel(sections, steps, outputs, *refs):
    place = position()
    fetched, out = refs[: sections - 1], refs[sections - 1]
    for mask in range(1, sections):
        way = jnp.where((place[0] ^ mask) > place[0], 0, 1)
        total = None
        for step in range(steps):
            term = contract(fetched[mask - 1][step], outputs[way, step], 0, 0)
            total = term if total is None else total + term
        out[mask - 1] = total


def weight_kernel(sections, steps, tokens, *refs):
    place = position()
    columns, halves, refs = refs[:2], refs[2:6], refs[6:]
    mirrored, lent, refs = refs[:2], refs[2:6], refs[6:]
    sent, refs = refs[: 2 * steps], refs[2 * steps :]
    own_slice, fetched, lent_slices = refs[0], refs[:sections], refs[sections - 1 :]
    out, lefts, rights, steers = refs[2 * sections - 1 :]
    width, head = out.shape[1:]
    every = 2 * steps * tokens
    lanes = pl.ds(pl.multiple_of(place[1] * width, 128), width)
    for index in range(2 * steps):
        rows = slice(index * tokens, (index + 1) * tokens)
        for way in range(2):
            for far in range(1, sections):
                steers[way, rows, (far - 1) * head : far * head] = sent[index][way, far]
            both = slice(way * every + index * tokens, way * every + (index + 1) * tokens)
            lefts[0, both, :] = sent[index][way, 0]
            lefts[1, both, :] = sent[index][way, sections]
        rights[rows, :] = columns[index // steps][index % steps, :, lanes]
        rows = slice(every + index * tokens, every + (index + 1) * tokens)
        rights[rows, :] = mirrored[index // steps][index % steps, :, lanes]
    out[0] = contract(lefts[0], rights[...], 0, 0).T
    for index in range(2 * steps):
        for way in range(2):
            both = slice(way * every + index * tokens, way * every + (index + 1) * tokens)

            @pl.when(place[3 + way] == place[1])
            def _():
                rights[both, :] = halves[2 * (index // steps) + way][index % steps]

            @pl.when(place[3 + way] != place[1])
            def _():
                rights[both, :] = lent[2 * (index // steps) + way][index % steps]

    def corrected(here, way):
        rows = slice(way * every, (way + 1) * every)
        blocks = []
        for far in range(1, sections - here):
            holder = here + far if way == 0 else sections - 1 - here - far
            if holder == here:
                blocks.append(own_slice[...])
            elif way == 1 and holder > here:
                blocks.append(lent_slices[holder ^ here][...])
            else:
                blocks.append(fetched[holder ^ here][place[2]])
        steer = steers[way, :, : len(blocks) * head]
        total = contract(steer, jnp.concatenate(blocks, axis=1), 1, 1)
        rights[rows, :] = (rights[rows, :].astype(jnp.float32) + total).astype(jnp.bfloat16)

    for here in range(sections - 1):

        @pl.when(place[0] == here)
        def _():
            for way in range(2):
                corrected(here, way)

    out[1] = contract(lefts[1], rights[...], 0, 0).T


def gathered(layer_inputs, saved_queries, saved_keys, held_weights, cotangent, valid_lengths):
    sections = lax.axis_size(SECTION)
    replicas = lax.axis_size("dp")
    steps = replicas // 2
    inputs = layer_inputs[0]
    held = held_weights[0]
    seqs, length, model_width = inputs.shape[1:]
    tokens = seqs * length
    head = held.shape[-1]
    width = model_width // replicas
    inputs = inputs.reshape(2, tokens, model_width)
    cot = cotangent.reshape(2, tokens, model_width)
    halved = held.reshape(2, 2, steps, 2, width, head)
    asides = (sections // 2, 1)
    memory = pl.BlockSpec(memory_space=pltpu.VMEM)
    scalars = pl.BlockSpec(memory_space=pltpu.SMEM)
    anywhere = pl.BlockSpec(memory_space=pl.ANY)
    hbm = pl.BlockSpec(memory_space=pltpu.HBM)

    picked = pl.pallas_call(
        functools.partial(pick_weights, sections),
        in_specs=[hbm],
        out_specs=[memory] * (sections - 1),
        out_shape=[jax.ShapeDtypeStruct((steps, width, head), jnp.bfloat16)] * (sections - 1),
        scratch_shapes=[pltpu.SemaphoreType.DMA((sections - 1,))],
        compiler_params=pltpu.CompilerParams(vmem_limit_bytes=52 << 20),
    )(halved)
    fetched = [None] * sections
    for mask in range(sections - 1, 0, -1):
        fetched[mask] = swapped(picked[mask - 1], SECTION, mask)

    wide = jax.ShapeDtypeStruct((2, tokens, 2 * width), jnp.bfloat16)
    slim = jax.ShapeDtypeStruct((2, tokens, width), jnp.bfloat16)
    picked = pl.pallas_call(
        functools.partial(pick_columns, steps, width),
        in_specs=[hbm] * 2,
        out_specs=[memory] * (2 * steps),
        out_shape=[wide] * steps + [slim] * steps,
        scratch_shapes=[pltpu.SemaphoreType.DMA((3 * steps,))],
        compiler_params=pltpu.CompilerParams(vmem_limit_bytes=52 << 20),
    )(inputs, cot)
    near_columns, near_halves = [picked[0]], [picked[steps]]
    for distance in range(1, steps):
        near_halves.append(shifted(picked[steps + distance], distance))
    for distance in range(1, steps):
        near_columns.append(shifted(picked[distance], distance))

    def moving(sources, which, shape):
        return pl.pallas_call(
            functools.partial(pick_moving, steps, which),
            in_specs=[anywhere] * steps,
            out_specs=[memory] * len(which),
            out_shape=[jax.ShapeDtypeStruct((steps,) + shape, jnp.bfloat16)] * len(which),
            scratch_shapes=[pltpu.SemaphoreType.DMA((steps * len(which),))],
            compiler_params=pltpu.CompilerParams(vmem_limit_bytes=8 << 20),
        )(*sources)

    sideways = moving(near_halves, (0, 1), (tokens, width))
    near_aside, far_aside, far_columns, far_halves = [], [], [], []
    for way in range(2):
        near_aside.append(swapped(sideways[way], SECTION, asides[way]))
    for way in range(2):
        far_aside.append(swapped(near_aside[way], "dp", 1))
    for way in range(2):
        far_halves.append(swapped(sideways[way], "dp", 1))

    lengths = valid_lengths
    blocks = 4
    cut = model_width // blocks
    short, full = pl.pallas_call(
        functools.partial(heads_kernel, length),
        grid=(blocks,),
        in_specs=[
            scalars,
            pl.BlockSpec((2, tokens, cut), lambda i: (0, 0, i)),
            pl.BlockSpec((2, tokens, cut), lambda i: (0, 0, i)),
            pl.BlockSpec((2, 2, cut, head), lambda i: (0, 0, i, 0)),
            pl.BlockSpec((2, tokens, head), lambda i: (0, 0, 0)),
            pl.BlockSpec((2, tokens, head), lambda i: (0, 0, 0)),
        ],
        out_specs=[pl.BlockSpec((rows * tokens, head), lambda i: (0, 0)) for rows in (3, 5)],
        out_shape=[jax.ShapeDtypeStruct((rows * tokens, head), jnp.bfloat16) for rows in (3, 5)],
        scratch_shapes=[pltpu.VMEM((2, 2, tokens, head), jnp.float32)],
        compiler_params=pltpu.CompilerParams(vmem_limit_bytes=12 << 20),
    )(
        lengths,
        inputs,
        cot,
        held,
        saved_queries[0].reshape(2, tokens, head),
        saved_keys[0].reshape(2, tokens, head),
    )

    tails = [full]
    for mask in range(1, sections):
        tails.append(swapped(full if mask == sections - 1 else short, SECTION, mask))

    outputs, own_values, own_slice = pl.pallas_call(
        pick_outputs,
        in_specs=[hbm, hbm],
        out_specs=[memory] * 3,
        out_shape=[
            jax.ShapeDtypeStruct((2, steps, width, head), jnp.bfloat16),
            jax.ShapeDtypeStruct((2, model_width, head), jnp.bfloat16),
            jax.ShapeDtypeStruct((width, head), jnp.bfloat16),
        ],
        scratch_shapes=[pltpu.SemaphoreType.DMA((3,))],
        compiler_params=pltpu.CompilerParams(vmem_limit_bytes=8 << 20),
    )(halved, held)
    products = pl.pallas_call(
        functools.partial(product_kernel, sections, steps),
        in_specs=[memory] * sections,
        out_specs=memory,
        out_shape=jax.ShapeDtypeStruct((sections - 1, head, head), jnp.float32),
        compiler_params=pltpu.CompilerParams(vmem_limit_bytes=8 << 20),
    )(outputs, *fetched[1:])
    far_products = swapped(products, "dp", 1)
    lent_back = [None] * sections
    for mask in range(1, sections):
        lent_back[mask] = swapped(fetched[mask], "dp", 1)

    packed = pl.pallas_call(
        pack_kernel,
        in_specs=[memory] * 2,
        out_specs=memory,
        out_shape=jax.ShapeDtypeStruct((sections - 1, head, head), jnp.bfloat16),
        compiler_params=pltpu.CompilerParams(vmem_limit_bytes=8 << 20),
    )(products, far_products)
    parts = [packed]
    for mask in range(1, sections):
        parts.append(swapped(packed, SECTION, mask))

    (upward,) = moving(near_columns, (1,), (tokens, 2 * width))
    near_mirror = swapped(upward, SECTION, sections - 1)
    far_mirror = swapped(near_mirror, "dp", 1)
    (downward,) = moving(near_columns, (0,), (tokens, 2 * width))
    far_columns = swapped(downward, "dp", 1)
    lent = [own_slice]
    for mask in range(1, sections):
        route = [
            (i, i ^ mask) for i in range(sections) if i ^ mask < i < sections - 1 - (i ^ mask)
        ]
        lent.append(lax.ppermute(own_slice, SECTION, route) if route else own_slice)

    sent, steer, own = pl.pallas_call(
        functools.partial(chain_kernel, sections, tokens, head),
        in_specs=[memory] * (2 * sections),
        out_specs=(memory, memory, memory),
        out_shape=(
            jax.ShapeDtypeStruct((2, sections + 1, tokens, head), jnp.bfloat16),
            jax.ShapeDtypeStruct((2 * tokens, (sections - 1) * head), jnp.bfloat16),
            jax.ShapeDtypeStruct((2, tokens, head), jnp.bfloat16),
        ),
        compiler_params=pltpu.CompilerParams(vmem_limit_bytes=8 << 20),
    )(*parts, *tails)

    near_sent = [sent]
    for distance in range(1, steps):
        near_sent.append(shifted(sent, distance))
    far_sent = []
    for distance in range(steps):
        far_sent.append(swapped(near_sent[distance], "dp", 1))

    grads_in = pl.pallas_call(
        functools.partial(input_kernel, sections, tokens),
        grid=(steps,),
        in_specs=[
            pl.BlockSpec((2, tokens, 2 * width), lambda i: (0, 0, i)),
            pl.BlockSpec((2 * tokens, (sections - 1) * head), lambda i: (0, 0)),
            pl.BlockSpec((2, tokens, head), lambda i: (0, 0, 0)),
            pl.BlockSpec((2, 2 * width, head), lambda i: (0, i, 0)),
        ]
        + [pl.BlockSpec((1, width, head), lambda i: (i, 0, 0))] * (2 * sections - 2),
        out_specs=pl.BlockSpec((2, tokens, 2 * width), lambda i: (0, 0, i)),
        out_shape=jax.ShapeDtypeStruct((2, tokens, model_width), jnp.bfloat16),
        compiler_params=pltpu.CompilerParams(vmem_limit_bytes=12 << 20),
    )(cot, steer, own, own_values, *fetched[1:], *lent_back[1:])

    every = replicas * tokens
    weight_grads = pl.pallas_call(
        functools.partial(weight_kernel, sections, steps, tokens),
        in_specs=[memory] * (2 * steps + 2 * sections + 11),
        out_specs=memory,
        out_shape=jax.ShapeDtypeStruct((2, width, head), jnp.float32),
        scratch_shapes=[
            pltpu.VMEM((2, 2 * every, head), jnp.bfloat16),
            pltpu.VMEM((2 * every, width), jnp.bfloat16),
            pltpu.VMEM((2, every, (sections - 1) * head), jnp.bfloat16),
        ],
        compiler_params=pltpu.CompilerParams(vmem_limit_bytes=20 << 20),
    )(
        downward,
        far_columns,
        *sideways,
        *far_halves,
        near_mirror,
        far_mirror,
        *near_aside,
        *far_aside,
        *near_sent,
        *far_sent,
        own_slice,
        *fetched[1:],
        *lent[1:],
    )
    shape = (1, 2, seqs, length, model_width)
    return (grads_in.reshape(shape), weight_grads[None])


def shards(*operands):
    layer_inputs, held_weights = operands[0], operands[3]
    sections = lax.axis_size(SECTION)
    replicas = lax.axis_size("dp")
    seqs, length, model_width = layer_inputs.shape[2:]
    head = held_weights.shape[-1]
    every_token = replicas * seqs * length
    moved = 2 * every_token * ((sections + 1) * head + 2 * model_width // replicas) * 2
    partial_sums = 4 * model_width * head * 4
    even = replicas % 2 == 0 and sections > 1 and sections & (sections - 1) == 0
    if even and moved < partial_sums and 2 * seqs * length <= head:
        return gathered(*operands)
    return reduced(*operands)


def solution(mesh):
    return jax.shard_map(
        shards,
        mesh=mesh,
        in_specs=(
            P(SECTION, None, "dp", None, None),
            P(SECTION, None, "dp", None, None),
            P(SECTION, None, "dp", None, None),
            P(SECTION, None, None, None, None),
            P(None, "dp", None, None),
            P(None, "dp"),
        ),
        out_specs=(P(SECTION, None, "dp", None, None), P(SECTION, None, "dp", None)),
        check_vma=False,
    )
```

```python
import functools
import math

import jax
import jax.numpy as jnp
from jax import lax
from jax.experimental import pallas as pl
from jax.experimental.pallas import tpu as pltpu
from jax.sharding import PartitionSpec as P


SECTION = "section"


def passed_along(block, axis, distance):
    devices = range(lax.axis_size(axis))
    route = [(i - distance, i) for i in devices if i - distance in devices]
    return lax.ppermute(block, axis, route)


def from_partner(block, axis, bit):
    count = lax.axis_size(axis)
    route = []
    for low in range(count):
        high = low | 1 << bit
        if high != low and high < count:
            route += [(low, high), (high, low)]
    return lax.ppermute(block, axis, route)


def attention_weights(queries, key_vectors, valid_lengths):
    length = queries.shape[-2]
    scores = jnp.einsum(
        "nmth,nmsh->nmts", queries, key_vectors, preferred_element_type=jnp.float32
    ) / math.sqrt(queries.shape[-1])
    row_pos = lax.broadcasted_iota(jnp.int32, (length, length), 0)
    col_pos = lax.broadcasted_iota(jnp.int32, (length, length), 1)
    allowed = (col_pos <= row_pos)[None, None] & (
        col_pos[None, None] < valid_lengths[:, :, None, None]
    )
    scores = jnp.where(allowed, scores, -jnp.inf)
    row_max = jnp.max(scores, axis=-1, keepdims=True)
    raised = jnp.where(allowed, jnp.exp(scores - row_max), 0.0)
    return (raised / jnp.sum(raised, axis=-1, keepdims=True)).astype(jnp.bfloat16)


def reduced(layer_inputs, saved_queries, saved_keys, held_weights, cotangent, valid_lengths):
    sections = lax.axis_size(SECTION)
    position = lax.axis_index(SECTION)
    inputs = layer_inputs[0]
    value_w = held_weights[0, :, 0]
    output_w = held_weights[0, :, 1]
    attend = attention_weights(saved_queries[0], saved_keys[0], valid_lengths)
    micro_count = inputs.shape[1]
    length = inputs.shape[2]
    model_width = inputs.shape[3]
    head_size = value_w.shape[2]
    values = jnp.einsum(
        "nmld,ndh->nmlh", inputs, value_w, preferred_element_type=jnp.float32
    ).astype(jnp.bfloat16)
    mixtures = jnp.einsum(
        "nmts,nmsh->nmth", attend, values, preferred_element_type=jnp.float32
    ).astype(jnp.bfloat16)
    is_end = [position == sections - 1, position == 0]
    starts = [sections - 1 - position, position]

    def make_compute(direction):

        def compute(operands):
            grads, uppers, vgrads, incoming, index = operands
            fresh = lax.dynamic_index_in_dim(cotangent[direction], index, 0, keepdims=False)
            upstream = jnp.where(is_end[direction], fresh, incoming)
            weights_now = lax.dynamic_index_in_dim(attend[direction], index, 0, keepdims=False)
            out_grad = jnp.dot(
                upstream, output_w[direction], preferred_element_type=jnp.float32
            ).astype(jnp.bfloat16)
            val_grad = jnp.einsum(
                "ts,th->sh", weights_now, out_grad, preferred_element_type=jnp.float32
            ).astype(jnp.bfloat16)
            branch = jnp.einsum(
                "lh,dh->ld", val_grad, value_w[direction], preferred_element_type=jnp.float32
            )
            grad_input = (upstream.astype(jnp.float32) + branch).astype(jnp.bfloat16)
            grads = lax.dynamic_update_index_in_dim(grads, grad_input, index, 0)
            uppers = lax.dynamic_update_index_in_dim(uppers, upstream, index, 0)
            vgrads = lax.dynamic_update_index_in_dim(vgrads, val_grad, index, 0)
            return (grad_input, (grads, uppers, vgrads))

        return compute

    def skip(operands):
        grads, uppers, vgrads, incoming, _ = operands
        return (jnp.zeros_like(incoming), (grads, uppers, vgrads))

    def advance(moment, received, buffers):
        outgoing = []
        updated = []
        for direction in range(2):
            micro_id = moment - starts[direction]
            active = (micro_id >= 0) & (micro_id < micro_count)
            clipped = jnp.clip(micro_id, 0, micro_count - 1)
            grads, uppers, vgrads = buffers[direction]
            sent_now, fresh_buffers = lax.cond(
                active,
                make_compute(direction),
                skip,
                (grads, uppers, vgrads, received[direction], clipped),
            )
            outgoing.append(sent_now)
            updated.append(fresh_buffers)
        return (jnp.stack(outgoing), tuple(updated))

    big_zero = jnp.zeros((micro_count, length, model_width), jnp.bfloat16)
    small_zero = jnp.zeros((micro_count, length, head_size), jnp.bfloat16)
    buffers = ((big_zero, big_zero, small_zero), (big_zero, big_zero, small_zero))
    sent, buffers = advance(
        jnp.int32(0), jnp.zeros((2, length, model_width), jnp.bfloat16), buffers
    )

    def loop_body(moment, carried):
        outgoing, held = carried
        from_next = passed_along(outgoing[0], SECTION, -1)
        from_prev = passed_along(outgoing[1], SECTION, 1)
        return advance(moment, jnp.stack([from_next, from_prev]), held)

    sent, buffers = lax.fori_loop(1, sections + micro_count - 1, loop_body, (sent, buffers))
    grads_in = jnp.stack([buffers[0][0], buffers[1][0]])
    upstreams = jnp.stack([buffers[0][1], buffers[1][1]])
    val_grads = jnp.stack([buffers[0][2], buffers[1][2]])
    flat_in = inputs.reshape(2, micro_count * length, model_width)
    flat_up = upstreams.reshape(2, micro_count * length, model_width)
    flat_mix = mixtures.reshape(2, micro_count * length, head_size)
    flat_vg = val_grads.reshape(2, micro_count * length, head_size)
    grad_value = jnp.einsum("ntd,nth->dnh", flat_in, flat_vg, preferred_element_type=jnp.float32)
    grad_output = jnp.einsum("ntd,nth->dnh", flat_up, flat_mix, preferred_element_type=jnp.float32)
    summed = lax.psum_scatter(
        jnp.stack([grad_value, grad_output], axis=2).reshape(
            model_width // lax.axis_size("dp") * lax.axis_size("dp"), 4 * head_size
        ),
        "dp",
        scatter_dimension=0,
        tiled=True,
    )
    summed = summed.reshape(-1, 2, 2, head_size)
    own_part = summed[:, 0]
    mirror_part = summed[:, 1]
    for bit_no in range(sections.bit_length() - 1):
        mirror_part = from_partner(mirror_part.astype(jnp.bfloat16), SECTION, bit_no).astype(
            mirror_part.dtype
        )
    combined = own_part + mirror_part
    weight_grads = jnp.transpose(combined, (1, 0, 2))[None]
    return (grads_in[None], weight_grads)


def swapped(block, axis, mask):
    return lax.ppermute(block, axis, [(i, i ^ mask) for i in range(lax.axis_size(axis))])


def shifted(block, distance):
    count = lax.axis_size("dp")
    return lax.ppermute(block, "dp", [(i, (i + 2 * distance) % count) for i in range(count)])


def contract(left, right, left_dim, right_dim):
    return lax.dot_general(
        left, right, (((left_dim,), (right_dim,)), ((), ())), preferred_element_type=jnp.float32
    )


def heads_kernel(length, valid, inputs, cot, held, queries, key_vectors, short, out, sums):
    tokens, head = queries.shape[1:]
    for way in range(2):
        for which, source in enumerate((inputs, cot)):
            term = contract(source[way], held[way, which], 1, 0)
            first = pl.program_id(0) == 0

            @pl.when(first)
            def _():
                sums[which, way] = term

            @pl.when(jnp.logical_not(first))
            def _():
                sums[which, way] += term

    @pl.when(pl.program_id(0) == pl.num_programs(0) - 1)
    def _():
        row = lax.broadcasted_iota(jnp.int32, (tokens, tokens), 0)
        col = lax.broadcasted_iota(jnp.int32, (tokens, tokens), 1)
        out[2 * tokens : 3 * tokens, :] = jnp.zeros((tokens, head), jnp.bfloat16)
        for way in range(2):
            scores = contract(queries[way], key_vectors[way], 1, 1) / math.sqrt(head)
            allowed = None
            for seq in range(tokens // length):
                start = seq * length
                here = (row >= start) & (row < start + length) & (col >= start) & (col <= row)
                here &= col - start < valid[way, seq]
                allowed = here if allowed is None else allowed | here
            scores = jnp.where(allowed, scores, -jnp.inf)
            row_max = jnp.max(scores, axis=-1, keepdims=True)
            raised = jnp.where(allowed, jnp.exp(scores - row_max), 0.0)
            attend = (raised / jnp.sum(raised, axis=-1, keepdims=True)).astype(jnp.bfloat16)
            mixture = contract(attend, sums[0, way].astype(jnp.bfloat16), 1, 0)
            out[way * tokens : (way + 1) * tokens, :] = sums[1, way].astype(jnp.bfloat16)
            out[2 * tokens : 3 * tokens, way * tokens : (way + 1) * tokens] = attend
            rows = slice((3 + way) * tokens, (4 + way) * tokens)
            out[rows, :] = mixture.astype(jnp.bfloat16)
        short[...] = out[: 3 * tokens, :]


def pack_kernel(near, far, out):
    out[...] = (near[...] + far[...]).astype(jnp.bfloat16)


def chain_kernel(sections, tokens, head, *refs):
    place = position()
    parts, tails = refs[:sections], refs[sections : 2 * sections]
    gathered, steer, own = refs[2 * sections :]

    def at(here):
        mine = [[None] * sections, [None] * sections]
        for way in range(2):
            order = range(sections - 1, -1, -1) if way == 0 else range(sections)
            done = []
            for holder in order:
                part, tail = parts[here ^ holder], tails[here ^ holder]
                total = tail[way * tokens : (way + 1) * tokens, :].astype(jnp.float32)
                for other in done:
                    total += contract(mine[way][other], part[(other ^ holder) - 1], 1, 0)
                weights = tail[2 * tokens : 3 * tokens, way * tokens : (way + 1) * tokens]
                mine[way][holder] = contract(weights, total.astype(jnp.bfloat16), 0, 0).astype(
                    jnp.bfloat16
                )
                done.append(holder)
        zero = jnp.zeros((tokens, head), jnp.bfloat16)
        for far in range(sections):
            inside = here + far < sections
            gathered[0, far] = mine[0][here + far] if inside else zero
            gathered[1, far] = mine[1][sections - 1 - here - far] if inside else zero
        mirror = here ^ (sections - 1)
        gathered[0, sections] = tails[0][3 * tokens : 4 * tokens, :]
        gathered[1, sections] = tails[here ^ mirror][4 * tokens : 5 * tokens, :]
        for way in range(2):
            own[way] = mine[way][here]
        for mask in range(1, sections):
            other = here ^ mask
            way = 0 if other > here else 1
            lanes = slice((mask - 1) * head, mask * head)
            steer[way * tokens : (way + 1) * tokens, lanes] = mine[way][other]
            steer[(1 - way) * tokens : (2 - way) * tokens, lanes] = zero

    for here in range(sections):

        @pl.when(place[0] == here)
        def _():
            at(here)


def input_kernel(sections, tokens, cot, steer, own, held, *refs):
    place = position()
    near, far = refs[: sections - 1], refs[sections - 1 : 2 * sections - 2]
    out = refs[2 * sections - 2]
    width = near[0].shape[1]
    core = place[1]
    for which, fetched in ((core, near), (1 - core, far)):
        start = pl.multiple_of(which * width, 128)
        weights = jnp.concatenate([block[0] for block in fetched], axis=1)
        total = contract(steer[...], weights, 1, 1)
        for way in range(2):
            branch = contract(own[way], held[way, pl.ds(start, width), :], 1, 1)
            branch += total[way * tokens : (way + 1) * tokens]
            base = cot[way, :, pl.ds(start, width)].astype(jnp.float32)
            out[way, :, pl.ds(start, width)] = (base + branch).astype(jnp.bfloat16)


def pick_weights(sections, halved, *refs):
    place = position()
    outs, sems = refs[: sections - 1], refs[sections - 1]
    here, core = place[0], place[1]
    copies = []
    for mask in range(sections - 1, 0, -1):
        way = jnp.where((here ^ mask) < here, 0, 1)
        copy = pltpu.make_async_copy(
            halved.at[way, 0, :, core], outs[mask - 1], sems.at[mask - 1]
        )
        copy.start()
        copies.append(copy)
    for copy in copies:
        copy.wait()


def position():
    here, replica = lax.axis_index(SECTION), lax.axis_index("dp")
    asides = (lax.axis_size(SECTION) // 2, 1)
    bits = [jnp.where((here & aside) != 0, 1, 0) for aside in asides]
    return (here, lax.rem(replica, 2), lax.div(replica, 2), *bits)


def carried_out(copies):
    for copy in copies:
        copy.start()
    for copy in copies:
        copy.wait()


def pick_outputs(halved, whole, out, own, part, sems):
    place = position()
    carried_out(
        [
            pltpu.make_async_copy(halved.at[1, 0, place[2], place[1]], part, sems.at[2]),
            pltpu.make_async_copy(halved.at[:, 1, :, place[1]], out, sems.at[0]),
            pltpu.make_async_copy(whole.at[:, 0], own, sems.at[1]),
        ]
    )


def pick_columns(steps, width, inputs, cot, *refs):
    place = position()
    outs, halves, sems = refs[:steps], refs[steps : 2 * steps], refs[2 * steps]
    copies = []
    for distance in range(steps):
        start = pl.multiple_of((place[2] + distance) % steps * 2 * width, 128)
        copies.append(
            pltpu.make_async_copy(
                inputs.at[:, :, pl.ds(start, 2 * width)], outs[distance], sems.at[3 * distance]
            )
        )
        for way in range(2):
            half = pl.multiple_of(start + place[3 + way] * width, 128)
            copies.append(
                pltpu.make_async_copy(
                    cot.at[way, :, pl.ds(half, width)],
                    halves[distance].at[way],
                    sems.at[3 * distance + 1 + way],
                )
            )
    carried_out(copies)


def pick_moving(steps, which, *refs):
    sources, outs, sems = refs[:steps], refs[steps:-1], refs[-1]
    copies = []
    for step, source in enumerate(sources):
        for index, out in zip(which, outs):
            copies.append(
                pltpu.make_async_copy(source.at[index], out.at[step], sems.at[len(copies)])
            )
    carried_out(copies)


def product_kernel(sections, steps, outputs, *refs):
    place = position()
    fetched, out = refs[: sections - 1], refs[sections - 1]
    for mask in range(1, sections):
        way = jnp.where((place[0] ^ mask) > place[0], 0, 1)
        total = None
        for step in range(steps):
            term = contract(fetched[mask - 1][step], outputs[way, step], 0, 0)
            total = term if total is None else total + term
        out[mask - 1] = total


def assemble_kernel(steps, tokens, *refs):
    place = position()
    columns, halves, mirrored, lent, outs = refs[:2], refs[2:6], refs[6:8], refs[8:12], refs[12:]
    width = outs[0].shape[-1]
    every = 2 * steps * tokens
    lanes = pl.ds(pl.multiple_of(place[1] * width, 128), width)
    for index in range(2 * steps):
        rows = slice(index * tokens, (index + 1) * tokens)
        outs[0][rows, :] = columns[index // steps][index % steps, :, lanes]
        rows = slice(every + index * tokens, every + (index + 1) * tokens)
        outs[0][rows, :] = mirrored[index // steps][index % steps, :, lanes]
        for way in range(2):
            both = slice(way * every + index * tokens, way * every + (index + 1) * tokens)

            @pl.when(place[3 + way] == place[1])
            def _():
                outs[1][both, :] = halves[2 * (index // steps) + way][index % steps]

            @pl.when(place[3 + way] != place[1])
            def _():
                outs[1][both, :] = lent[2 * (index // steps) + way][index % steps]


def weight_kernel(sections, steps, tokens, *refs):
    place = position()
    inputs, cots, refs = refs[0], refs[1], refs[2:]
    sent, refs = refs[: 2 * steps], refs[2 * steps :]
    own_slice, fetched, lent_slices = refs[0], refs[:sections], refs[sections - 1 :]
    out, lefts, rights, steers = refs[2 * sections - 1 :]
    _, head = out.shape[1:]
    every = 2 * steps * tokens
    for index in range(2 * steps):
        rows = slice(index * tokens, (index + 1) * tokens)
        for way in range(2):
            for far in range(1, sections):
                steers[way, rows, (far - 1) * head : far * head] = sent[index][way, far]
            both = slice(way * every + index * tokens, way * every + (index + 1) * tokens)
            lefts[0, both, :] = sent[index][way, 0]
            lefts[1, both, :] = sent[index][way, sections]
    out[0] = contract(lefts[0], inputs[...], 0, 0).T

    def corrected(here, way):
        rows = slice(way * every, (way + 1) * every)
        blocks = []
        for far in range(1, sections - here):
            holder = here + far if way == 0 else sections - 1 - here - far
            if holder == here:
                blocks.append(own_slice[...])
            elif way == 1 and holder > here:
                blocks.append(lent_slices[holder ^ here][...])
            else:
                blocks.append(fetched[holder ^ here][place[2]])
        steer = steers[way, :, : len(blocks) * head]
        total = contract(steer, jnp.concatenate(blocks, axis=1), 1, 1)
        rights[rows, :] = (cots[rows, :].astype(jnp.float32) + total).astype(jnp.bfloat16)

    @pl.when(place[0] == sections - 1)
    def _():
        rights[...] = cots[...]

    for here in range(sections - 1):

        @pl.when(place[0] == here)
        def _():
            for way in range(2):
                corrected(here, way)

    out[1] = contract(lefts[1], rights[...], 0, 0).T


def gathered(layer_inputs, saved_queries, saved_keys, held_weights, cotangent, valid_lengths):
    sections = lax.axis_size(SECTION)
    replicas = lax.axis_size("dp")
    steps = replicas // 2
    inputs = layer_inputs[0]
    held = held_weights[0]
    seqs, length, model_width = inputs.shape[1:]
    tokens = seqs * length
    head = held.shape[-1]
    width = model_width // replicas
    inputs = inputs.reshape(2, tokens, model_width)
    cot = cotangent.reshape(2, tokens, model_width)
    halved = held.reshape(2, 2, steps, 2, width, head)
    asides = (sections // 2, 1)
    memory = pl.BlockSpec(memory_space=pltpu.VMEM)
    scalars = pl.BlockSpec(memory_space=pltpu.SMEM)
    anywhere = pl.BlockSpec(memory_space=pl.ANY)
    hbm = pl.BlockSpec(memory_space=pltpu.HBM)

    picked = pl.pallas_call(
        functools.partial(pick_weights, sections),
        in_specs=[hbm],
        out_specs=[memory] * (sections - 1),
        out_shape=[jax.ShapeDtypeStruct((steps, width, head), jnp.bfloat16)] * (sections - 1),
        scratch_shapes=[pltpu.SemaphoreType.DMA((sections - 1,))],
        compiler_params=pltpu.CompilerParams(vmem_limit_bytes=52 << 20),
    )(halved)
    fetched = [None] * sections
    for mask in range(sections - 1, 0, -1):
        fetched[mask] = swapped(picked[mask - 1], SECTION, mask)

    wide = jax.ShapeDtypeStruct((2, tokens, 2 * width), jnp.bfloat16)
    slim = jax.ShapeDtypeStruct((2, tokens, width), jnp.bfloat16)
    picked = pl.pallas_call(
        functools.partial(pick_columns, steps, width),
        in_specs=[hbm] * 2,
        out_specs=[memory] * (2 * steps),
        out_shape=[wide] * steps + [slim] * steps,
        scratch_shapes=[pltpu.SemaphoreType.DMA((3 * steps,))],
        compiler_params=pltpu.CompilerParams(vmem_limit_bytes=52 << 20),
    )(inputs, cot)
    near_columns, near_halves = [picked[0]], [picked[steps]]
    for distance in range(1, steps):
        near_halves.append(shifted(picked[steps + distance], distance))
    for distance in range(1, steps):
        near_columns.append(shifted(picked[distance], distance))

    def moving(sources, which, shape):
        return pl.pallas_call(
            functools.partial(pick_moving, steps, which),
            in_specs=[anywhere] * steps,
            out_specs=[memory] * len(which),
            out_shape=[jax.ShapeDtypeStruct((steps,) + shape, jnp.bfloat16)] * len(which),
            scratch_shapes=[pltpu.SemaphoreType.DMA((steps * len(which),))],
            compiler_params=pltpu.CompilerParams(vmem_limit_bytes=8 << 20),
        )(*sources)

    sideways = moving(near_halves, (0, 1), (tokens, width))
    near_aside, far_aside, far_columns, far_halves = [], [], [], []
    for way in range(2):
        near_aside.append(swapped(sideways[way], SECTION, asides[way]))
    for way in range(2):
        far_aside.append(swapped(near_aside[way], "dp", 1))
    for way in range(2):
        far_halves.append(swapped(sideways[way], "dp", 1))

    lengths = valid_lengths
    blocks = 4
    cut = model_width // blocks
    short, full = pl.pallas_call(
        functools.partial(heads_kernel, length),
        grid=(blocks,),
        in_specs=[
            scalars,
            pl.BlockSpec((2, tokens, cut), lambda i: (0, 0, i)),
            pl.BlockSpec((2, tokens, cut), lambda i: (0, 0, i)),
            pl.BlockSpec((2, 2, cut, head), lambda i: (0, 0, i, 0)),
            pl.BlockSpec((2, tokens, head), lambda i: (0, 0, 0)),
            pl.BlockSpec((2, tokens, head), lambda i: (0, 0, 0)),
        ],
        out_specs=[pl.BlockSpec((rows * tokens, head), lambda i: (0, 0)) for rows in (3, 5)],
        out_shape=[jax.ShapeDtypeStruct((rows * tokens, head), jnp.bfloat16) for rows in (3, 5)],
        scratch_shapes=[pltpu.VMEM((2, 2, tokens, head), jnp.float32)],
        compiler_params=pltpu.CompilerParams(vmem_limit_bytes=12 << 20),
    )(
        lengths,
        inputs,
        cot,
        held,
        saved_queries[0].reshape(2, tokens, head),
        saved_keys[0].reshape(2, tokens, head),
    )

    tails = [full]
    for mask in range(1, sections):
        tails.append(swapped(full if mask == sections - 1 else short, SECTION, mask))

    outputs, own_values, own_slice = pl.pallas_call(
        pick_outputs,
        in_specs=[hbm, hbm],
        out_specs=[memory] * 3,
        out_shape=[
            jax.ShapeDtypeStruct((2, steps, width, head), jnp.bfloat16),
            jax.ShapeDtypeStruct((2, model_width, head), jnp.bfloat16),
            jax.ShapeDtypeStruct((width, head), jnp.bfloat16),
        ],
        scratch_shapes=[pltpu.SemaphoreType.DMA((3,))],
        compiler_params=pltpu.CompilerParams(vmem_limit_bytes=8 << 20),
    )(halved, held)
    products = pl.pallas_call(
        functools.partial(product_kernel, sections, steps),
        in_specs=[memory] * sections,
        out_specs=memory,
        out_shape=jax.ShapeDtypeStruct((sections - 1, head, head), jnp.float32),
        compiler_params=pltpu.CompilerParams(vmem_limit_bytes=8 << 20),
    )(outputs, *fetched[1:])
    far_products = swapped(products, "dp", 1)
    lent_back = [None] * sections
    for mask in range(1, sections):
        lent_back[mask] = swapped(fetched[mask], "dp", 1)

    packed = pl.pallas_call(
        pack_kernel,
        in_specs=[memory] * 2,
        out_specs=memory,
        out_shape=jax.ShapeDtypeStruct((sections - 1, head, head), jnp.bfloat16),
        compiler_params=pltpu.CompilerParams(vmem_limit_bytes=8 << 20),
    )(products, far_products)
    parts = [packed]
    for mask in range(1, sections):
        parts.append(swapped(packed, SECTION, mask))

    (upward,) = moving(near_columns, (1,), (tokens, 2 * width))
    near_mirror = swapped(upward, SECTION, sections - 1)
    far_mirror = swapped(near_mirror, "dp", 1)
    (downward,) = moving(near_columns, (0,), (tokens, 2 * width))
    far_columns = swapped(downward, "dp", 1)
    lent = [own_slice]
    for mask in range(1, sections):
        route = [
            (i, i ^ mask) for i in range(sections) if i ^ mask < i < sections - 1 - (i ^ mask)
        ]
        lent.append(lax.ppermute(own_slice, SECTION, route) if route else own_slice)

    sent, steer, own = pl.pallas_call(
        functools.partial(chain_kernel, sections, tokens, head),
        in_specs=[memory] * (2 * sections),
        out_specs=(memory, memory, memory),
        out_shape=(
            jax.ShapeDtypeStruct((2, sections + 1, tokens, head), jnp.bfloat16),
            jax.ShapeDtypeStruct((2 * tokens, (sections - 1) * head), jnp.bfloat16),
            jax.ShapeDtypeStruct((2, tokens, head), jnp.bfloat16),
        ),
        compiler_params=pltpu.CompilerParams(vmem_limit_bytes=8 << 20),
    )(*parts, *tails)

    near_sent = [sent]
    for distance in range(1, steps):
        near_sent.append(shifted(sent, distance))
    far_sent = []
    for distance in range(steps):
        far_sent.append(swapped(near_sent[distance], "dp", 1))

    grads_in = pl.pallas_call(
        functools.partial(input_kernel, sections, tokens),
        grid=(steps,),
        in_specs=[
            pl.BlockSpec((2, tokens, 2 * width), lambda i: (0, 0, i)),
            pl.BlockSpec((2 * tokens, (sections - 1) * head), lambda i: (0, 0)),
            pl.BlockSpec((2, tokens, head), lambda i: (0, 0, 0)),
            pl.BlockSpec((2, 2 * width, head), lambda i: (0, i, 0)),
        ]
        + [pl.BlockSpec((1, width, head), lambda i: (i, 0, 0))] * (2 * sections - 2),
        out_specs=pl.BlockSpec((2, tokens, 2 * width), lambda i: (0, 0, i)),
        out_shape=jax.ShapeDtypeStruct((2, tokens, model_width), jnp.bfloat16),
        compiler_params=pltpu.CompilerParams(vmem_limit_bytes=12 << 20),
    )(cot, steer, own, own_values, *fetched[1:], *lent_back[1:])

    every = replicas * tokens
    assembled = pl.pallas_call(
        functools.partial(assemble_kernel, steps, tokens),
        in_specs=[memory] * 12,
        out_specs=[memory] * 2,
        out_shape=[jax.ShapeDtypeStruct((2 * every, width), jnp.bfloat16)] * 2,
        compiler_params=pltpu.CompilerParams(vmem_limit_bytes=12 << 20),
    )(
        downward,
        far_columns,
        *sideways,
        *far_halves,
        near_mirror,
        far_mirror,
        *near_aside,
        *far_aside,
    )
    weight_grads = pl.pallas_call(
        functools.partial(weight_kernel, sections, steps, tokens),
        in_specs=[memory] * (2 * steps + 2 * sections + 1),
        out_specs=memory,
        out_shape=jax.ShapeDtypeStruct((2, width, head), jnp.float32),
        scratch_shapes=[
            pltpu.VMEM((2, 2 * every, head), jnp.bfloat16),
            pltpu.VMEM((2 * every, width), jnp.bfloat16),
            pltpu.VMEM((2, every, (sections - 1) * head), jnp.bfloat16),
        ],
        compiler_params=pltpu.CompilerParams(vmem_limit_bytes=20 << 20),
    )(
        *assembled,
        *near_sent,
        *far_sent,
        own_slice,
        *fetched[1:],
        *lent[1:],
    )
    shape = (1, 2, seqs, length, model_width)
    return (grads_in.reshape(shape), weight_grads[None])


def shards(*operands):
    layer_inputs, held_weights = operands[0], operands[3]
    sections = lax.axis_size(SECTION)
    replicas = lax.axis_size("dp")
    seqs, length, model_width = layer_inputs.shape[2:]
    head = held_weights.shape[-1]
    every_token = replicas * seqs * length
    moved = 2 * every_token * ((sections + 1) * head + 2 * model_width // replicas) * 2
    partial_sums = 4 * model_width * head * 4
    even = replicas % 2 == 0 and sections > 1 and sections & (sections - 1) == 0
    if even and moved < partial_sums and 2 * seqs * length <= head:
        return gathered(*operands)
    return reduced(*operands)


def solution(mesh):
    return jax.shard_map(
        shards,
        mesh=mesh,
        in_specs=(
            P(SECTION, None, "dp", None, None),
            P(SECTION, None, "dp", None, None),
            P(SECTION, None, "dp", None, None),
            P(SECTION, None, None, None, None),
            P(None, "dp", None, None),
            P(None, "dp"),
        ),
        out_specs=(P(SECTION, None, "dp", None, None), P(SECTION, None, "dp", None)),
        check_vma=False,
    )
```
